32 devices in a mesh: dp: 8 (over z, y), dap: 4 (over x, core).
Axes of the slice: x: 2, y: 2, z: 4, core: 2. Of those that a mesh axis runs over, the one named last changes fastest.
Arguments:
- single_rep: bfloat16 [8, 128, 384], P('dp', 'dap')
- pair_rep: bfloat16 [8, 128, 128, 256], P('dp', 'dap')
- token_mask: int32 [8, 128], P('dp')
- d_single_out: bfloat16 [8, 128, 384], P('dp', 'dap')
- d_pair_out: bfloat16 [8, 128, 128, 256], P('dp', 'dap')
- mul_out_in: bfloat16 [256, 1024], replicated
- mul_out_gate: bfloat16 [256, 256], replicated
- mul_out_proj: bfloat16 [256, 256], replicated
- mul_in_in: bfloat16 [256, 1024], replicated
- mul_in_gate: bfloat16 [256, 256], replicated
- mul_in_proj: bfloat16 [256, 256], replicated
- att_st_qkvg: bfloat16 [256, 1024], replicated
- att_st_bias: bfloat16 [256, 8], replicated
- att_st_proj: bfloat16 [256, 256], replicated
- att_en_qkvg: bfloat16 [256, 1024], replicated
- att_en_bias: bfloat16 [256, 8], replicated
- att_en_proj: bfloat16 [256, 256], replicated
- pair_up: bfloat16 [256, 2048], replicated
- pair_down: bfloat16 [1024, 256], replicated
- sing_qkvg: bfloat16 [384, 1536], replicated
- sing_qbias: bfloat16 [384], replicated
- sing_pbias: bfloat16 [256, 16], replicated
- sing_proj: bfloat16 [384, 384], replicated
- sing_up: bfloat16 [384, 3072], replicated
- sing_down: bfloat16 [1536, 384], replicated
Outputs:
- output 1: bfloat16 [8, 128, 384], P('dp', 'dap')
- output 2: bfloat16 [8, 128, 128, 256], P('dp', 'dap')
- output 3: bfloat16 [8, 128, 384], P('dp', 'dap')
- output 4: bfloat16 [8, 128, 128, 256], P('dp', 'dap')
- output 5: float32 [4743552], P('dp')
All inputs are finite; a program needn't handle non-finite values.
Results may differ from the reference program's by a relative error of at most 0.02.
Values are sent between devices in bfloat16 or wider.
A program may use at most 1 GiB of HBM per device.

```python
import jax
import jax.numpy as jnp
from jax import lax

BATCH = 8
TOKENS = 128
C_S = 384
C_Z = 256
HEADS_S = 16
HEAD_S = 24
TRI_HEADS = 8
TRI_HEAD = 32
C_MUL = 256

NORM_EPS = 1e-5
MASK_PENALTY = 1.0e9


def weight_shapes():
    tri_width = TRI_HEADS * TRI_HEAD
    single_width = HEADS_S * HEAD_S
    return [
        ('mul_out_in', (C_Z, 4 * C_MUL), C_Z),
        ('mul_out_gate', (C_Z, C_Z), C_Z),
        ('mul_out_proj', (C_MUL, C_Z), C_MUL),
        ('mul_in_in', (C_Z, 4 * C_MUL), C_Z),
        ('mul_in_gate', (C_Z, C_Z), C_Z),
        ('mul_in_proj', (C_MUL, C_Z), C_MUL),
        ('att_st_qkvg', (C_Z, 4 * tri_width), C_Z),
        ('att_st_bias', (C_Z, TRI_HEADS), C_Z),
        ('att_st_proj', (tri_width, C_Z), tri_width),
        ('att_en_qkvg', (C_Z, 4 * tri_width), C_Z),
        ('att_en_bias', (C_Z, TRI_HEADS), C_Z),
        ('att_en_proj', (tri_width, C_Z), tri_width),
        ('pair_up', (C_Z, 8 * C_Z), C_Z),
        ('pair_down', (4 * C_Z, C_Z), 4 * C_Z),
        ('sing_qkvg', (C_S, 4 * single_width), C_S),
        ('sing_qbias', (single_width,), 1),
        ('sing_pbias', (C_Z, HEADS_S), C_Z),
        ('sing_proj', (single_width, C_S), single_width),
        ('sing_up', (C_S, 8 * C_S), C_S),
        ('sing_down', (4 * C_S, C_S), 4 * C_S),
    ]


def setup_inputs(seed: int = 0) -> dict:
    base_key = jax.random.key(seed)
    key_list = jax.random.split(base_key, 32)
    lengths = jax.random.randint(key_list[0], (BATCH,), TOKENS // 4, TOKENS + 1)
    full_pick = jax.random.randint(key_list[1], (), 0, BATCH)
    lengths = jnp.where(jnp.arange(BATCH) == full_pick, TOKENS, lengths)
    inputs = {}
    inputs['single_rep'] = jax.random.normal(key_list[2], (BATCH, TOKENS, C_S), jnp.float32).astype(jnp.bfloat16)
    inputs['pair_rep'] = jax.random.normal(key_list[3], (BATCH, TOKENS, TOKENS, C_Z), jnp.float32).astype(jnp.bfloat16)
    inputs['token_mask'] = (jnp.arange(TOKENS)[None, :] < lengths[:, None]).astype(jnp.int32)
    inputs['d_single_out'] = jax.random.normal(key_list[4], (BATCH, TOKENS, C_S), jnp.float32).astype(jnp.bfloat16)
    inputs['d_pair_out'] = jax.random.normal(key_list[5], (BATCH, TOKENS, TOKENS, C_Z), jnp.float32).astype(jnp.bfloat16)
    for w_index, (w_name, w_shape, fan_in) in enumerate(weight_shapes()):
        w_draw = jax.random.normal(key_list[6 + w_index], w_shape, jnp.float32)
        inputs[w_name] = (w_draw * fan_in ** -0.5).astype(jnp.bfloat16)
    return inputs


def layer_norm(x_in):
    x_f32 = x_in.astype(jnp.float32)
    centered = x_f32 - jnp.mean(x_f32, axis=-1, keepdims=True)
    row_var = jnp.mean(centered * centered, axis=-1, keepdims=True)
    return centered * lax.rsqrt(row_var + NORM_EPS)


def tri_mul(z_one, w_in, w_gate, w_out, mix_form):
    normed = layer_norm(z_one).astype(jnp.bfloat16)
    proj_all = jnp.dot(normed, w_in, preferred_element_type=jnp.float32)
    left_proj = (jax.nn.sigmoid(proj_all[..., C_MUL:2 * C_MUL]) * proj_all[..., :C_MUL]).astype(jnp.bfloat16)
    right_proj = (jax.nn.sigmoid(proj_all[..., 3 * C_MUL:]) * proj_all[..., 2 * C_MUL:3 * C_MUL]).astype(jnp.bfloat16)
    gate_vals = jax.nn.sigmoid(jnp.dot(normed, w_gate, preferred_element_type=jnp.float32))
    mixed_sum = jnp.einsum(mix_form, left_proj.astype(jnp.float32), right_proj.astype(jnp.float32))
    mixed_norm = layer_norm(mixed_sum).astype(jnp.bfloat16)
    update = gate_vals * jnp.dot(mixed_norm, w_out, preferred_element_type=jnp.float32)
    return (z_one.astype(jnp.float32) + update).astype(jnp.bfloat16)


def tri_att(z_one, mask_bias, w_qkvg, w_tb, w_o):
    normed = layer_norm(z_one).astype(jnp.bfloat16)
    proj_all = jnp.dot(normed, w_qkvg, preferred_element_type=jnp.float32)
    tri_width = TRI_HEADS * TRI_HEAD
    head_shape = (TOKENS, TOKENS, TRI_HEADS, TRI_HEAD)
    q_all = proj_all[..., :tri_width].astype(jnp.bfloat16).reshape(head_shape)
    k_all = proj_all[..., tri_width:2 * tri_width].astype(jnp.bfloat16).reshape(head_shape)
    v_all = proj_all[..., 2 * tri_width:3 * tri_width].astype(jnp.bfloat16).reshape(head_shape)
    gate_vals = jax.nn.sigmoid(proj_all[..., 3 * tri_width:])
    bias_hjk = jnp.transpose(jnp.dot(normed, w_tb, preferred_element_type=jnp.float32).astype(jnp.bfloat16), (2, 0, 1)).astype(jnp.float32)
    att_scale = TRI_HEAD ** -0.5

    def one_row(row_item):
        q_row, k_row, v_row = row_item
        logits = jnp.einsum('jhd,khd->hjk', q_row.astype(jnp.float32), k_row.astype(jnp.float32)) * att_scale + bias_hjk + mask_bias
        prob_mat = jax.nn.softmax(logits, axis=-1).astype(jnp.bfloat16)
        return jnp.einsum('hjk,khd->jhd', prob_mat.astype(jnp.float32), v_row.astype(jnp.float32))

    attended = lax.map(one_row, (q_all, k_all, v_all))
    gated = (gate_vals * attended.reshape(TOKENS, TOKENS, tri_width)).astype(jnp.bfloat16)
    return (z_one.astype(jnp.float32) + jnp.dot(gated, w_o, preferred_element_type=jnp.float32)).astype(jnp.bfloat16)


def transition(x_rows, w_up, w_down):
    normed = layer_norm(x_rows).astype(jnp.bfloat16)
    hidden = jnp.dot(normed, w_up, preferred_element_type=jnp.float32)
    inner_dim = w_down.shape[0]
    acted = (jax.nn.silu(hidden[..., :inner_dim]) * hidden[..., inner_dim:]).astype(jnp.bfloat16)
    return (x_rows.astype(jnp.float32) + jnp.dot(acted, w_down, preferred_element_type=jnp.float32)).astype(jnp.bfloat16)


def single_att(s_one, z_one, mask_bias, w_qkvg, q_bias, w_pb, w_o):
    normed = layer_norm(s_one).astype(jnp.bfloat16)
    proj_all = jnp.dot(normed, w_qkvg, preferred_element_type=jnp.float32)
    single_width = HEADS_S * HEAD_S
    head_shape = (TOKENS, HEADS_S, HEAD_S)
    q_all = (proj_all[:, :single_width] + q_bias.astype(jnp.float32)).astype(jnp.bfloat16).reshape(head_shape)
    k_all = proj_all[:, single_width:2 * single_width].astype(jnp.bfloat16).reshape(head_shape)
    v_all = proj_all[:, 2 * single_width:3 * single_width].astype(jnp.bfloat16).reshape(head_shape)
    gate_vals = jax.nn.sigmoid(proj_all[:, 3 * single_width:])
    pair_norm = layer_norm(z_one).astype(jnp.bfloat16)
    bias_all = jnp.dot(pair_norm, w_pb, preferred_element_type=jnp.float32).astype(jnp.bfloat16)
    logits = jnp.einsum('ihd,jhd->hij', q_all.astype(jnp.float32), k_all.astype(jnp.float32)) * HEAD_S ** -0.5
    logits = logits + jnp.transpose(bias_all, (2, 0, 1)).astype(jnp.float32) + mask_bias
    prob_mat = jax.nn.softmax(logits, axis=-1).astype(jnp.bfloat16)
    attended = jnp.einsum('hij,jhd->ihd', prob_mat.astype(jnp.float32), v_all.astype(jnp.float32))
    gated = (gate_vals * attended.reshape(TOKENS, single_width)).astype(jnp.bfloat16)
    return (s_one.astype(jnp.float32) + jnp.dot(gated, w_o, preferred_element_type=jnp.float32)).astype(jnp.bfloat16)


def block_forward(s_one, z_one, mask_one, params):
    w_list = [p_item.astype(jnp.bfloat16) for p_item in params]
    mask_bias = (mask_one.astype(jnp.float32) - 1.0) * MASK_PENALTY
    z_val = tri_mul(z_one, w_list[0], w_list[1], w_list[2], 'ikc,jkc->ijc')
    z_val = tri_mul(z_val, w_list[3], w_list[4], w_list[5], 'kic,kjc->ijc')
    z_val = tri_att(z_val, mask_bias, w_list[6], w_list[7], w_list[8])
    z_val = jnp.transpose(tri_att(jnp.transpose(z_val, (1, 0, 2)), mask_bias, w_list[9], w_list[10], w_list[11]), (1, 0, 2))
    z_val = transition(z_val, w_list[12], w_list[13])
    s_val = single_att(s_one, z_val, mask_bias, w_list[14], w_list[15], w_list[16], w_list[17])
    s_val = transition(s_val, w_list[18], w_list[19])
    return s_val, z_val


def reference(single_rep, pair_rep, token_mask, d_single_out, d_pair_out, mul_out_in, mul_out_gate, mul_out_proj, mul_in_in, mul_in_gate, mul_in_proj, att_st_qkvg, att_st_bias, att_st_proj, att_en_qkvg, att_en_bias, att_en_proj, pair_up, pair_down, sing_qkvg, sing_qbias, sing_pbias, sing_proj, sing_up, sing_down):
    weights = (mul_out_in, mul_out_gate, mul_out_proj, mul_in_in, mul_in_gate, mul_in_proj, att_st_qkvg, att_st_bias, att_st_proj, att_en_qkvg, att_en_bias, att_en_proj, pair_up, pair_down, sing_qkvg, sing_qbias, sing_pbias, sing_proj, sing_up, sing_down)
    params = tuple(w_item.astype(jnp.float32) for w_item in weights)

    def scan_step(grad_acc, scan_item):
        s_one, z_one, mask_one, gs_one, gz_one = scan_item

        def forward_one(s_val, z_val, p_val):
            return block_forward(s_val, z_val, mask_one, p_val)

        outs_one, pull_back = jax.vjp(forward_one, s_one, z_one, params)
        ds_one, dz_one, grad_one = pull_back((gs_one, gz_one))
        new_acc = tuple(acc_item + grad_item for acc_item, grad_item in zip(grad_acc, grad_one))
        return new_acc, (outs_one[0], outs_one[1], ds_one, dz_one)

    init_acc = tuple(jnp.zeros_like(p_item) for p_item in params)
    grad_sums, stacked = lax.scan(scan_step, init_acc, (single_rep, pair_rep, token_mask, d_single_out, d_pair_out))
    grad_flat = jnp.concatenate([g_item.reshape(-1) for g_item in grad_sums])
    return stacked[0], stacked[1], stacked[2], stacked[3], grad_flat
```

```python
import functools
import jax
import jax.numpy as jnp
from jax import lax
from jax.experimental import pallas as pl
from jax.experimental.pallas import tpu as pltpu
from jax.sharding import PartitionSpec as P


BATCH_AXIS = 'dp'
GROUP_AXIS = 'dap'
MASK_PENALTY = 1.0e9
NCH = 4
WORK = 1 << 12

NORM_EPS = 1e-5
F32 = jnp.float32
BF16 = jnp.bfloat16


def mm(a, b):
    return lax.dot_general(a, b, (((1,), (0,)), ((), ())), preferred_element_type=F32)


def mm_nt(a, b):
    return lax.dot_general(a, b, (((1,), (1,)), ((), ())), preferred_element_type=F32)


def mm_tn(a, b):
    return lax.dot_general(a, b, (((0,), (0,)), ((), ())), preferred_element_type=F32)


def ln_stats(x):
    inv = 1.0 / x.shape[-1]
    c = x - jnp.sum(x, axis=-1, keepdims=True) * inv
    r = lax.rsqrt(jnp.sum(c * c, axis=-1, keepdims=True) * inv + NORM_EPS)
    return c * r, r


def ln_back(dn, xh, r):
    inv = 1.0 / dn.shape[-1]
    m1 = jnp.sum(dn, axis=-1, keepdims=True) * inv
    m2 = jnp.sum(dn * xh, axis=-1, keepdims=True) * inv
    return r * (dn - m1 - xh * m2)


def put_flat(ref, val):
    n = val.shape[1] // 128
    for t in range(n):
        ref[pl.ds(t, val.shape[0], stride=n), :] = val[:, t * 128:(t + 1) * 128]


def flat_shape(w):
    return jax.ShapeDtypeStruct((w.size // 128, 128), F32)


def last_step():
    return pl.program_id(0) == pl.num_programs(0) - 1


def sig(x):
    return 1.0 / (1.0 + jnp.exp(-x))


def trans_fwd_body(z_ref, wu_ref, wd_ref, o_ref):
    x = z_ref[...].astype(F32)
    xh, _ = ln_stats(x)
    h = mm(xh.astype(BF16), wu_ref[...])
    d = h.shape[1] // 2
    h1 = h[:, :d]
    act = (h1 * sig(h1) * h[:, d:]).astype(BF16)
    o_ref[...] = (x + mm(act, wd_ref[...])).astype(BF16)


def trans_bwd_body(z_ref, g_ref, wu_ref, wd_ref, dz_ref, fu_ref, fd_ref, dwu_ref, dwd_ref):
    @pl.when(pl.program_id(0) == 0)
    def _():
        dwu_ref[...] = jnp.zeros_like(dwu_ref)
        dwd_ref[...] = jnp.zeros_like(dwd_ref)

    x = z_ref[...].astype(F32)
    xh, r = ln_stats(x)
    n = xh.astype(BF16)
    h = mm(n, wu_ref[...])
    d = h.shape[1] // 2
    h1, h2 = h[:, :d], h[:, d:]
    s = sig(h1)
    sl = h1 * s
    act = (sl * h2).astype(BF16)
    g = g_ref[...]
    da = mm_nt(g, wd_ref[...]).astype(BF16).astype(F32)
    dwd_ref[...] += mm_tn(act, g)
    dh1 = (da * h2 * (s + sl * (1.0 - s))).astype(BF16)
    dh2 = (da * sl).astype(BF16)
    dh = jnp.concatenate([dh1, dh2], axis=1)
    dwu_ref[...] += mm_tn(n, dh)
    dn = mm_nt(dh, wu_ref[...])
    dz_ref[...] = (g.astype(F32) + ln_back(dn, xh, r)).astype(BF16)

    @pl.when(last_step())
    def _():
        put_flat(fu_ref, dwu_ref[...])
        put_flat(fd_ref, dwd_ref[...])


def row_spec(b):
    return pl.BlockSpec((b, T, C), lambda i: (i, 0, 0))


def full(a):
    nd = len(a.shape)
    return pl.BlockSpec(a.shape, lambda i: (0,) * nd)


def cp(flops):
    return dict(cost_estimate=pl.CostEstimate(flops=flops, bytes_accessed=1 << 23, transcendentals=0),
                compiler_params=pltpu.CompilerParams(vmem_limit_bytes=60 << 20, dimension_semantics=("arbitrary",)))


def trans_fwd(z, wu, wd, blk):
    p, c = z.shape
    spec = pl.BlockSpec((blk, c), lambda i: (i, 0))
    return pl.pallas_call(trans_fwd_body, grid=(p // blk,), in_specs=[spec, full(wu), full(wd)], out_specs=spec,
                          out_shape=jax.ShapeDtypeStruct((p, c), BF16), name="trans_fwd", **cp(p * c * WORK))(z, wu, wd)


def trans_bwd(z, g, wu, wd, blk):
    p, c = z.shape
    spec = pl.BlockSpec((blk, c), lambda i: (i, 0))
    return pl.pallas_call(trans_bwd_body, grid=(p // blk,), in_specs=[spec, spec, full(wu), full(wd)],
                          out_specs=[spec, full(flat_shape(wu)), full(flat_shape(wd))],
                          out_shape=[jax.ShapeDtypeStruct((p, c), BF16), flat_shape(wu), flat_shape(wd)],
                          scratch_shapes=[pltpu.VMEM(wu.shape, F32), pltpu.VMEM(wd.shape, F32)],
                          name="trans_bwd", **cp(p * c * WORK))(z, g, wu, wd)


H = 8
D = 32
T = 128
C = 256


def head_masks(width, dim):
    lane = lax.broadcasted_iota(jnp.int32, (1, width), 1)
    return [((lane >= h * dim) & (lane < (h + 1) * dim)).astype(F32).astype(BF16) for h in range(width // dim)]


def pair_setup():
    masks = head_masks(C, D)
    n = H // 2
    lane = lax.broadcasted_iota(jnp.int32, (1, C), 1)
    low = (lane < T).astype(F32).astype(BF16)
    return [a + b for a, b in zip(masks[:n], masks[n:])], [low, 1 - low]


def row_masks():
    row = lax.broadcasted_iota(jnp.int32, (C, 1), 0) // D % (H // 2)
    return [(row == m).astype(F32).astype(BF16) for m in range(H // 2)]


def unpair(x, pairs):
    return sum(x[m * T:(m + 1) * T] * p.astype(F32) for m, p in enumerate(pairs))


def head_tn(x, w, flips):
    xt = x.astype(F32).T.astype(BF16)
    y = mm(jnp.concatenate([xt * f for f in flips], axis=1), w)
    return jnp.concatenate([y[:T, :T], y[T:, T:]]).T.astype(BF16)


def softmax(s):
    e = jnp.exp(s - jnp.max(s, axis=-1, keepdims=True))
    return e * (1.0 / jnp.sum(e, axis=-1, keepdims=True))


def stack_heads(x, masks):
    return jnp.concatenate([x * m for m in masks])


def bias_body(z_ref, wbt_ref, o_ref):
    for i in range(z_ref.shape[0]):
        xh, _ = ln_stats(z_ref[i].astype(F32))
        o_ref[i] = mm_nt(wbt_ref[...], xh.astype(BF16)).astype(BF16)


def att_bias(z3, wbt):
    r, h = z3.shape[0], wbt.shape[0]
    return pl.pallas_call(bias_body, grid=(r // 8,), in_specs=[row_spec(8), full(wbt)],
                          out_specs=pl.BlockSpec((8, h, T), lambda i: (i, 0, 0)),
                          out_shape=jax.ShapeDtypeStruct((r, h, T), BF16), name="att_bias", **cp(r * T * C * WORK))(z3, wbt)


def att_fwd_body(z_ref, bias_ref, wq_ref, wo_ref, o_ref):
    b = z_ref.shape[0]
    pairs, sides = pair_setup()
    x = z_ref[...].reshape(b * T, C).astype(F32)
    xh, _ = ln_stats(x)
    pr = mm(xh.astype(BF16), wq_ref[...])
    gates = sig(pr[:, 3 * C:])
    prb = pr[:, :3 * C].astype(BF16)
    outs = []
    for i in range(b):
        row = prb[i * T:(i + 1) * T]
        q, k, v = row[:, :C], row[:, C:2 * C], row[:, 2 * C:]
        lg = mm_nt(stack_heads(q, pairs), stack_heads(k, sides)) * (D ** -0.5)
        ps = []
        for m in range(len(pairs)):
            s = lg[m * T:(m + 1) * T]
            ps.append(jnp.concatenate([softmax(s[:, :T] + bias_ref[m]), softmax(s[:, T:] + bias_ref[m + len(pairs)])], axis=1).astype(BF16))
        o = unpair(mm(jnp.concatenate(ps), stack_heads(v, sides)), pairs)
        outs.append((gates[i * T:(i + 1) * T] * o).astype(BF16))
    gated = jnp.concatenate(outs)
    o_ref[...] = (x + mm(gated, wo_ref[...])).astype(BF16).reshape(b, T, C)


def att_fwd(z3, bias, wq, wo, b):
    r = z3.shape[0]
    spec = row_spec(b)
    return pl.pallas_call(att_fwd_body, grid=(r // b,), in_specs=[spec, full(bias), full(wq), full(wo)], out_specs=spec,
                          out_shape=jax.ShapeDtypeStruct((r, T, C), BF16), name="att_fwd",
                          **cp(r * T * C * WORK))(z3, bias, wq, wo)


def att_bwd_body(z_ref, g_ref, bias_ref, wq_ref, wo_ref, dn_ref, dbias_ref, fq_ref, fo_ref, dwq_ref, dwo_ref):
    @pl.when(pl.program_id(0) == 0)
    def _():
        dbias_ref[...] = jnp.zeros_like(dbias_ref)
        dwq_ref[...] = jnp.zeros_like(dwq_ref)
        dwo_ref[...] = jnp.zeros_like(dwo_ref)

    b = z_ref.shape[0]
    pairs, sides = pair_setup()
    flips = row_masks()
    x = z_ref[...].reshape(b * T, C).astype(F32)
    g = g_ref[...].reshape(b * T, C)
    xh, _ = ln_stats(x)
    n = xh.astype(BF16)
    pr = mm(n, wq_ref[...])
    gates = sig(pr[:, 3 * C:])
    prb = pr[:, :3 * C].astype(BF16)
    dgd = mm_nt(g, wo_ref[...]).astype(BF16).astype(F32)
    do_all = (dgd * gates).astype(BF16)
    gat, dps = [], []
    for i in range(b):
        sl = slice(i * T, (i + 1) * T)
        row = prb[sl]
        q, k, v = row[:, :C], row[:, C:2 * C], row[:, 2 * C:]
        do = do_all[sl]
        qs, dos = stack_heads(q, pairs), stack_heads(do, pairs)
        kk, vv = stack_heads(k, sides), stack_heads(v, sides)
        lg = mm_nt(qs, kk) * (D ** -0.5)
        dp = mm_nt(dos, vv)
        ps, ds = [], []
        for m in range(len(pairs)):
            pp, dd = [], []
            for e in range(2):
                h = m + e * len(pairs)
                blk = (slice(m * T, (m + 1) * T), slice(e * T, (e + 1) * T))
                p = softmax(lg[blk] + bias_ref[h])
                pd = p * dp[blk].astype(BF16).astype(F32)
                dsh = pd - p * jnp.sum(pd, axis=-1, keepdims=True)
                dbias_ref[h] += dsh
                pp.append(p.astype(BF16))
                dd.append((dsh * (D ** -0.5)).astype(BF16))
            ps.append(jnp.concatenate(pp, axis=1))
            ds.append(jnp.concatenate(dd, axis=1))
        ps, ds = jnp.concatenate(ps), jnp.concatenate(ds)
        o = unpair(mm(ps, vv), pairs)
        dq = unpair(mm(ds, kk), pairs).astype(BF16)
        dk, dv = head_tn(q, ds, flips), head_tn(do, ps, flips)
        gt = gates[sl]
        gat.append((gt * o).astype(BF16))
        dgl = (dgd[sl] * o * gt * (1.0 - gt)).astype(BF16)
        dps.append(jnp.concatenate([dq, dk, dv, dgl], axis=1))
    gated = jnp.concatenate(gat)
    dpr = jnp.concatenate(dps)
    dwo_ref[...] += mm_tn(gated, g)
    dwq_ref[...] += mm_tn(n, dpr)
    dn_ref[...] = mm_nt(dpr, wq_ref[...])

    @pl.when(last_step())
    def _():
        put_flat(fq_ref, dwq_ref[...])
        put_flat(fo_ref, dwo_ref[...])


def att_bwd(z3, g3, bias, wq, wo, b):
    r = z3.shape[0]
    spec = row_spec(b)
    return pl.pallas_call(att_bwd_body, grid=(r // b,), in_specs=[spec, spec, full(bias), full(wq), full(wo)],
                          out_specs=[pl.BlockSpec((b * T, C), lambda i: (i, 0)), full(bias), full(flat_shape(wq)), full(flat_shape(wo))],
                          out_shape=[jax.ShapeDtypeStruct((r * T, C), F32), jax.ShapeDtypeStruct(bias.shape, F32), flat_shape(wq), flat_shape(wo)],
                          scratch_shapes=[pltpu.VMEM(wq.shape, F32), pltpu.VMEM(wo.shape, F32)],
                          name="att_bwd", **cp(r * T * C * WORK))(z3, g3, bias, wq, wo)


def att_fin_body(z_ref, g_ref, db_ref, wbt_ref, *rest):
    dz_ref, dwbt_ref = rest[-2:]

    @pl.when(pl.program_id(0) == 0)
    def _():
        dwbt_ref[...] = jnp.zeros_like(dwbt_ref)

    b = z_ref.shape[0]
    xh, r = ln_stats(z_ref[...].reshape(b * T, C).astype(F32))
    n = xh.astype(BF16)
    parts = []
    for i in range(b):
        db = db_ref[i].astype(BF16)
        parts.append(mm_tn(db, wbt_ref[...]))
        dwbt_ref[...] += mm(db, n[i * T:(i + 1) * T])
    dn = jnp.concatenate(parts)
    if len(rest) == 3:
        dn = dn + rest[0][...]
    dz_ref[...] = (g_ref[...].reshape(b * T, C).astype(F32) + ln_back(dn, xh, r)).astype(BF16).reshape(b, T, C)


def att_fin(z3, g3, db, wbt, dn=None):
    r, h = z3.shape[0], wbt.shape[0]
    b = 8
    spec = row_spec(b)
    extra = [] if dn is None else [dn]
    return pl.pallas_call(att_fin_body, grid=(r // b,),
                          in_specs=[spec, spec, pl.BlockSpec((b, h, T), lambda i: (i, 0, 0)), full(wbt)]
                          + [pl.BlockSpec((b * T, C), lambda i: (i, 0))] * len(extra),
                          out_specs=[spec, full(wbt)],
                          out_shape=[jax.ShapeDtypeStruct((r, T, C), BF16), jax.ShapeDtypeStruct(wbt.shape, F32)],
                          name="att_fin", **cp(r * T * C * WORK))(z3, g3, db, wbt, *extra)


RB = 16
CB = 32


def put_row(scr, i, val):
    scr[pl.ds(i, val.shape[0], stride=RB), :] = val


def get_row(scr, i, n):
    return scr[pl.ds(i, n, stride=RB), :]


def cspecs(n):
    return [pl.BlockSpec((C // n, RB, T), lambda i: (0, i, 0))] * n


def cshapes(n, r, dt=BF16):
    return [jax.ShapeDtypeStruct((C // n, r, T), dt)] * n


def flush(scr, refs):
    w = C // len(refs)
    for p, ref in enumerate(refs):
        ref[...] = scr[pl.ds(p * w * RB, w * RB), :].reshape(w, RB, T).astype(BF16)


def mul_pre_body(z_ref, wt_ref, *rest):
    outs, sa, sb = rest[:-2], rest[-2], rest[-1]
    wt = wt_ref[...]
    for i in range(0, RB, 2):
        xh, _ = ln_stats(z_ref[i:i + 2].reshape(2 * T, C).astype(F32))
        pt = mm_nt(wt, xh.astype(BF16))
        at = sig(pt[C:2 * C]) * pt[:C]
        bt = sig(pt[3 * C:]) * pt[2 * C:3 * C]
        for e in range(2):
            put_row(sa, i + e, at[:, e * T:(e + 1) * T])
            put_row(sb, i + e, bt[:, e * T:(e + 1) * T])
    flush(sa, outs[:NCH])
    flush(sb, outs[NCH:])


def mul_pre(z3, wt):
    r = z3.shape[0]
    zs = row_spec(RB)
    out = pl.pallas_call(mul_pre_body, grid=(r // RB,), in_specs=[zs, full(wt)], out_specs=cspecs(NCH) * 2, out_shape=cshapes(NCH, r) * 2,
                         scratch_shapes=[pltpu.VMEM((C * RB, T), F32)] * 2, name="mul_pre", **cp(r * T * C * WORK))(z3, wt)
    return out[:NCH], out[NCH:]


def collect(idx_ref, refs, buf):
    for rel, ref in enumerate(refs):
        r = ref.shape[1]
        buf[:, pl.ds(pl.multiple_of(idx_ref[rel] * r, r), r), :] = ref[...]


def mix_call(body, idx, ins, n_out, out_dt, n_buf):
    w, r, _ = ins[0].shape
    spec = pl.BlockSpec((CB, r, T), lambda i, s: (i, 0, 0))
    gs = pltpu.PrefetchScalarGridSpec(num_scalar_prefetch=1, grid=(w // CB,), in_specs=[spec] * len(ins), out_specs=[spec] * n_out,
                                      scratch_shapes=[pltpu.VMEM((CB, T, T), BF16)] * n_buf)
    return pl.pallas_call(body, grid_spec=gs, out_shape=[jax.ShapeDtypeStruct((w, r, T), out_dt)] * n_out, **cp(r * w * T * WORK))(idx, *ins)


def mix_fwd_body(idx_ref, a_ref, b0, b1, b2, b3, x_ref, buf):
    collect(idx_ref, (b0, b1, b2, b3), buf)
    for c in range(CB):
        x_ref[c] = mm_nt(a_ref[c], buf[c])


def mix_fwd(idx, a, b4):
    return mix_call(mix_fwd_body, idx, [a, *b4], 1, F32, 1)[0]


def mix_bwd_out_body(idx_ref, dx_ref, dt_ref, b0, b1, b2, b3, a0, a1, a2, a3, da_ref, db_ref, bb, ab):
    collect(idx_ref, (b0, b1, b2, b3), bb)
    collect(idx_ref, (a0, a1, a2, a3), ab)
    for c in range(CB):
        da_ref[c] = mm(dx_ref[c], bb[c]).astype(BF16)
        db_ref[c] = mm(dt_ref[c], ab[c]).astype(BF16)


def mix_bwd_out(idx, dx, dxt, b4, a4):
    return mix_call(mix_bwd_out_body, idx, [dx, dxt, *b4, *a4], 2, BF16, 2)


def mix_bwd_in_body(idx_ref, a_ref, b_ref, d0, d1, d2, d3, da_ref, db_ref, buf):
    collect(idx_ref, (d0, d1, d2, d3), buf)
    for c in range(CB):
        d = buf[c]
        da_ref[c] = mm_nt(b_ref[c], d).astype(BF16)
        db_ref[c] = mm(a_ref[c], d).astype(BF16)


def mix_bwd_in(idx, d4, a, b):
    return mix_call(mix_bwd_in_body, idx, [a, b, *d4], 2, BF16, 1)


def ln0_stats(x):
    inv = 1.0 / x.shape[0]
    c = x - jnp.sum(x, axis=0, keepdims=True) * inv
    r = lax.rsqrt(jnp.sum(c * c, axis=0, keepdims=True) * inv + NORM_EPS)
    return c * r, r


def ln0_back(dn, xh, r):
    inv = 1.0 / dn.shape[0]
    m1 = jnp.sum(dn, axis=0, keepdims=True) * inv
    m2 = jnp.sum(dn * xh, axis=0, keepdims=True) * inv
    return r * (dn - m1 - xh * m2)


def col_of(refs, i):
    return jnp.concatenate([ref[:, i, :] for ref in refs])


def mul_post_body(*refs):
    xs, (z_ref, wg_ref, wo_ref, o_ref) = refs[:NCH], refs[NCH:]
    for i in range(z_ref.shape[0]):
        z = z_ref[i].astype(F32)
        n, _ = ln_stats(z)
        g = sig(mm(n.astype(BF16), wg_ref[...]))
        xn, _ = ln0_stats(col_of(xs, i))
        o_ref[i] = (z + g * mm_tn(xn.astype(BF16), wo_ref[...])).astype(BF16)


def mul_post(xs, z3, wg, wo):
    r = z3.shape[0]
    b = 8
    zs = row_spec(b)
    xspec = pl.BlockSpec((C // NCH, b, T), lambda i: (0, i, 0))
    return pl.pallas_call(mul_post_body, grid=(r // b,), in_specs=[xspec] * NCH + [zs, full(wg), full(wo)],
                          out_specs=zs, out_shape=jax.ShapeDtypeStruct((r, T, C), BF16), name="mul_post", **cp(r * T * C * WORK))(*xs, z3, wg, wo)


def mul_post_bwd_body(pix, *refs):
    xs, (z_ref, d_ref, wg_ref, wo_ref) = refs[:NCH], refs[NCH:NCH + 4]
    dxs, (dgl_ref, fo_ref) = refs[NCH + 4:2 * NCH + 4], refs[2 * NCH + 4:2 * NCH + 6]
    scr, dwo_ref = refs[-2:]

    @pl.when(pl.program_id(0) == 0)
    def _():
        dwo_ref[...] = jnp.zeros_like(dwo_ref)

    for i in range(RB):
        n, _ = ln_stats(z_ref[i].astype(F32))
        g = sig(mm(n.astype(BF16), wg_ref[...]))
        xh, r = ln0_stats(col_of(xs, i))
        xn = xh.astype(BF16)
        u = mm_tn(xn, wo_ref[...])
        d = d_ref[i].astype(F32)
        du = (d * g).astype(BF16)
        dgl_ref[i] = (d * u * g * (1.0 - g)).astype(BF16)
        dwo_ref[...] += mm(xn, du)
        dx = ln0_back(mm_nt(wo_ref[...], du), xh, r)
        put_row(scr, i, dx)
        if pix:
            refs[2 * NCH + 6][i] = dx.T.astype(BF16)
    flush(scr, dxs)

    @pl.when(last_step())
    def _():
        put_flat(fo_ref, dwo_ref[...])


def mul_post_bwd(xs, z3, d3, wg, wo, pix):
    r = z3.shape[0]
    zs = row_spec(RB)
    zsh = jax.ShapeDtypeStruct((r, T, C), BF16)
    out = pl.pallas_call(functools.partial(mul_post_bwd_body, pix), grid=(r // RB,), in_specs=cspecs(NCH) + [zs, zs, full(wg), full(wo)],
                         out_specs=cspecs(NCH) + [zs, full(flat_shape(wo))] + [zs] * pix,
                         out_shape=cshapes(NCH, r) + [zsh, flat_shape(wo)] + [zsh] * pix,
                         scratch_shapes=[pltpu.VMEM((C * RB, T), F32), pltpu.VMEM(wo.shape, F32)],
                         name="mul_post_bwd", **cp(r * T * C * WORK))(*xs, z3, d3, wg, wo)
    return (out[:NCH], *out[NCH:])


def flip_body(d_ref, *rest):
    sin, sout = rest[-2:]
    for hf in range(2):
        sin[hf] = d_ref[:, :, hf * T:(hf + 1) * T].astype(F32).reshape(T * RB, T)
    for j in range(RB):
        for hf in range(2):
            m = sin[hf, pl.ds(j, T, stride=RB), :]
            sout[pl.ds(hf * T * RB + j, T, stride=RB), :] = m.T
    flush(sout, rest[:-2])


def flip(d):
    r = d.shape[1]
    return pl.pallas_call(flip_body, grid=(r // RB,), in_specs=[pl.BlockSpec((T, RB, C), lambda i: (0, i, 0))],
                          out_specs=cspecs(NCH), out_shape=cshapes(NCH, r),
                          scratch_shapes=[pltpu.VMEM((2, T * RB, T), F32), pltpu.VMEM((C * RB, T), F32)], name="flip", **cp(r * T * C * WORK))(d)


def load_all(scr, refs):
    w = C // len(refs)
    for p, ref in enumerate(refs):
        scr[pl.ds(p * w * RB, w * RB), :] = ref[...].astype(F32).reshape(w * RB, T)


def mul_pre_bwd_body(*refs):
    das, dbs = refs[:NCH], refs[NCH:2 * NCH]
    z_ref, g_ref, dgl_ref, w_ref, wt_ref, wg_ref, dz_ref, fi_ref, fg_ref, sa, sb, dwt_ref, dwg_ref = refs[2 * NCH:]

    @pl.when(pl.program_id(0) == 0)
    def _():
        dwt_ref[...] = jnp.zeros_like(dwt_ref)
        dwg_ref[...] = jnp.zeros_like(dwg_ref)

    load_all(sa, das)
    load_all(sb, dbs)
    for i in range(0, RB, 2):
        xh, r = ln_stats(z_ref[i:i + 2].reshape(2 * T, C).astype(F32))
        n = xh.astype(BF16)
        pt = mm_nt(wt_ref[...], n)
        da = jnp.concatenate([get_row(sa, i, C), get_row(sa, i + 1, C)], axis=1)
        db = jnp.concatenate([get_row(sb, i, C), get_row(sb, i + 1, C)], axis=1)
        s1, s2 = sig(pt[C:2 * C]), sig(pt[3 * C:])
        d1, d3 = da * s1, db * s2
        dp = jnp.concatenate([d1.astype(BF16), (d1 * pt[:C] * (1.0 - s1)).astype(BF16),
                              d3.astype(BF16), (d3 * pt[2 * C:3 * C] * (1.0 - s2)).astype(BF16)])
        dgl = dgl_ref[i:i + 2].reshape(2 * T, C)
        dwt_ref[...] += mm(dp, n)
        dwg_ref[...] += mm_tn(n, dgl)
        dn = mm(w_ref[...], dp).T + mm_nt(dgl, wg_ref[...])
        dz = g_ref[i:i + 2].reshape(2 * T, C).astype(F32) + ln_back(dn, xh, r)
        dz_ref[i:i + 2] = dz.astype(BF16).reshape(2, T, C)

    @pl.when(last_step())
    def _():
        put_flat(fi_ref, dwt_ref[...].T)
        put_flat(fg_ref, dwg_ref[...])


def mul_pre_bwd(z3, g3, das, dbs, dgl, w, wt, wg):
    r = z3.shape[0]
    zs = row_spec(RB)
    return pl.pallas_call(mul_pre_bwd_body, grid=(r // RB,), in_specs=cspecs(NCH) * 2 + [zs, zs, zs, full(w), full(wt), full(wg)],
                          out_specs=[zs, full(flat_shape(wt)), full(flat_shape(wg))],
                          out_shape=[jax.ShapeDtypeStruct((r, T, C), BF16), flat_shape(wt), flat_shape(wg)],
                          scratch_shapes=[pltpu.VMEM((C * RB, T), F32)] * 2 + [pltpu.VMEM(wt.shape, F32), pltpu.VMEM(wg.shape, F32)],
                          name="mul_pre_bwd", **cp(r * T * C * WORK))(*das, *dbs, z3, g3, dgl, w, wt, wg)


SH = 16
SD = 24


def single_body(s_ref, d_ref, bias_ref, wq_ref, qb_ref, wo_ref, wu_ref, wd_ref,
                so_ref, ds_ref, dbias_ref, dqb_ref, dwq_ref, dwo_ref, dwu_ref, dwd_ref):
    w = s_ref.shape[1]
    masks = head_masks(w, SD)
    x = s_ref[...].astype(F32)
    xh, r = ln_stats(x)
    n = xh.astype(BF16)
    pr = mm(n, wq_ref[...])
    q = (pr[:, :w] + qb_ref[...].astype(F32)).astype(BF16)
    k = pr[:, w:2 * w].astype(BF16)
    v = pr[:, 2 * w:3 * w].astype(BF16)
    gt = sig(pr[:, 3 * w:])
    qs = stack_heads(q, masks)
    lg = mm_nt(qs, k) * (SD ** -0.5)
    pf, ps = [], []
    for h in range(SH):
        p = softmax(lg[h * T:(h + 1) * T] + bias_ref[h].T)
        pf.append(p)
        ps.append(p.astype(BF16))
    o = mm(jnp.concatenate(ps, axis=1), stack_heads(v, masks))
    gated = (gt * o).astype(BF16)
    s1 = (x + mm(gated, wo_ref[...])).astype(BF16)
    x1 = s1.astype(F32)
    xh1, r1 = ln_stats(x1)
    n1 = xh1.astype(BF16)
    hid = mm(n1, wu_ref[...])
    d = hid.shape[1] // 2
    h1, h2 = hid[:, :d], hid[:, d:]
    sg = sig(h1)
    sl = h1 * sg
    act = (sl * h2).astype(BF16)
    so_ref[...] = (x1 + mm(act, wd_ref[...])).astype(BF16)
    g = d_ref[...]
    da = mm_nt(g, wd_ref[...]).astype(BF16).astype(F32)
    put_flat(dwd_ref, mm_tn(act, g))
    dh = jnp.concatenate([(da * h2 * (sg + sl * (1.0 - sg))).astype(BF16), (da * sl).astype(BF16)], axis=1)
    put_flat(dwu_ref, mm_tn(n1, dh))
    g1 = (g.astype(F32) + ln_back(mm_nt(dh, wu_ref[...]), xh1, r1)).astype(BF16)
    dgd = mm_nt(g1, wo_ref[...]).astype(BF16).astype(F32)
    put_flat(dwo_ref, mm_tn(gated, g1))
    do = (dgd * gt).astype(BF16)
    dgl = (dgd * o * gt * (1.0 - gt)).astype(BF16)
    dos = stack_heads(do, masks)
    dp = mm_nt(dos, v)
    ds = []
    for h in range(SH):
        pd = pf[h] * dp[h * T:(h + 1) * T].astype(BF16).astype(F32)
        dsh = pd - pf[h] * jnp.sum(pd, axis=-1, keepdims=True)
        dbias_ref[h] = dsh.T
        ds.append((dsh * (SD ** -0.5)).astype(BF16))
    dq = mm(jnp.concatenate(ds, axis=1), stack_heads(k, masks)).astype(BF16)
    dk = mm_tn(jnp.concatenate(ds), qs).astype(BF16)
    dv = mm_tn(jnp.concatenate(ps), dos).astype(BF16)
    dqb_ref[...] = jnp.sum(dq.astype(F32), axis=0, keepdims=True)
    dpr = jnp.concatenate([dq, dk, dv, dgl], axis=1)
    put_flat(dwq_ref, mm_tn(n, dpr))
    ds_ref[...] = (g1.astype(F32) + ln_back(mm_nt(dpr, wq_ref[...]), xh, r)).astype(BF16)


def single_step(s, d, bias, wq, qb, wo, wu, wd):
    vm = pl.BlockSpec(memory_space=pltpu.VMEM)
    sh = [jax.ShapeDtypeStruct(s.shape, BF16)] * 2 + [jax.ShapeDtypeStruct(a.shape, F32) for a in (bias, qb)] + [flat_shape(a) for a in (wq, wo, wu, wd)]
    return pl.pallas_call(single_body, in_specs=[vm] * 8, out_specs=[vm] * 8, out_shape=sh, name="single_step",
                          cost_estimate=pl.CostEstimate(flops=1 << 33, bytes_accessed=1 << 24, transcendentals=0),
                          compiler_params=pltpu.CompilerParams(vmem_limit_bytes=60 << 20))(s, d, bias, wq, qb, wo, wu, wd)


def flip_perm(bit):
    return [(i, i ^ bit) for i in range(4)]


def swap_core(x_in):
    return lax.ppermute(x_in, GROUP_AXIS, flip_perm(1))


def swap_chip(x_in):
    return lax.ppermute(x_in, GROUP_AXIS, flip_perm(2))


def gather_rel(xs):
    out = []
    for x_in in xs:
        near = swap_core(x_in)
        far = swap_chip(x_in)
        out.append((x_in, near, far, swap_core(far)))
    return out


def mix_all(fn, *chunks):
    out = []
    for args in zip(*chunks):
        out.append(fn(*args))
    return out


def rows_to_cols(x_in):
    return jnp.transpose(lax.all_to_all(x_in, GROUP_AXIS, 1, 0, tiled=True), (1, 0, 2))


def cols_to_rows(x_in):
    return lax.all_to_all(jnp.transpose(x_in, (1, 0, 2)), GROUP_AXIS, 0, 1, tiled=True)


def scatter_rows(x_in):
    me = lax.axis_index(GROUP_AXIS)
    chip, core = me // 2, me % 2
    halves = x_in.reshape((2, 2) + (x_in.shape[0] // 4,) + x_in.shape[1:])
    mine = lax.dynamic_index_in_dim(halves, chip, 0, keepdims=False)
    mine = mine + swap_chip(lax.dynamic_index_in_dim(halves, 1 - chip, 0, keepdims=False))
    own = lax.dynamic_index_in_dim(mine, core, 0, keepdims=False)
    return own + swap_core(lax.dynamic_index_in_dim(mine, 1 - core, 0, keepdims=False))


def bias_full(part, mask_add):
    return jnp.transpose(lax.all_gather(part, GROUP_AXIS, axis=0, tiled=True), (1, 0, 2)).astype(F32) + mask_add


def group_half(pieces, partial):
    core = lax.axis_index(GROUP_AXIS) % 2
    rows = sum(p.shape[0] for p in pieces)
    pad = -rows % 128
    flat = jnp.concatenate(list(pieces) + ([jnp.zeros((pad, 128), F32)] if pad else []), axis=0)
    half = flat.shape[0] // 2
    mine = lax.dynamic_slice_in_dim(flat, core * half, half)
    if partial:
        mine = mine + swap_core(lax.dynamic_slice_in_dim(flat, (1 - core) * half, half))
    return mine


def scatter_group(mine):
    return lax.psum_scatter(mine, BATCH_AXIS, scatter_dimension=0, tiled=True)


def gather_group(part, partial):
    if partial:
        part = part + swap_chip(part)
    got = lax.all_gather(part, BATCH_AXIS, axis=0, tiled=True)
    return got, swap_core(got)


def dp_perm(bit):
    n = lax.axis_size(BATCH_AXIS)
    return [(i, i ^ bit) for i in range(n)]


def small_group(mine):
    me = lax.axis_index(BATCH_AXIS)
    bits = (1, 2, 4)
    for bit in bits:
        half = mine.shape[0] // 2
        side = (me // bit) % 2
        other = lax.ppermute(lax.dynamic_slice_in_dim(mine, (1 - side) * half, half), BATCH_AXIS, dp_perm(bit))
        mine = lax.dynamic_slice_in_dim(mine, side * half, half) + other
    mine = mine + swap_chip(mine)
    for bit in reversed(bits):
        half = mine.shape[0]
        side = (me // bit) % 2
        other = lax.ppermute(mine, BATCH_AXIS, dp_perm(bit))
        both = jnp.zeros((2 * half, 128), F32)
        both = lax.dynamic_update_slice_in_dim(both, mine, side * half, 0)
        mine = lax.dynamic_update_slice_in_dim(both, other, (1 - side) * half, 0)
    return mine, swap_core(mine)


def chunk_pieces(table, start, size, core):
    at, out = 0, []
    for elems, group, row, flip_dim, half in table:
        lo, hi = max(at, start), min(at + elems, start + size)
        if lo < hi:
            cut = half * 128
            a, b = row * 128 + lo - at, row * 128 + hi - at
            if flip_dim:
                a, b = row * 128, row * 128 + elems
            spans = [(a, min(b, cut)), (max(a, cut), b)]
            segs = [(group, int((base >= cut) != (core == 1)), base % cut, end - base) for base, end in spans if base < end]
            out.append((segs, flip_dim, lo - at, hi - at))
        at += elems
    return out


def assemble(table, groups, total):
    n = lax.axis_size(BATCH_AXIS)
    part = total // n

    def branch(d, core):
        def run(*flat_groups):
            res = []
            for segs, flip_dim, lo, hi in chunk_pieces(table, d * part, part, core):
                vals = [flat_groups[2 * g + side].reshape(-1)[o:o + ln] for g, side, o, ln in segs]
                if flip_dim:
                    val = jnp.concatenate(vals).reshape(flip_dim, -1).T.reshape(-1)
                    vals = [val[lo:hi]]
                res += vals
            return jnp.concatenate(res)

        return run

    which = lax.axis_index(BATCH_AXIS) * 2 + lax.axis_index(GROUP_AXIS) % 2
    flat_groups = [a for g in groups for a in g]
    return lax.switch(which, [branch(d, c) for d in range(n) for c in range(2)], *flat_groups)


def tie(*vals):
    return lax.optimization_barrier(vals)


ORDER = ("1i", "1g", "1o", "2i", "2g", "2o", "3q", "3b", "3o", "4q", "4b", "4o", "pu", "pd", "sq", "sb", "sp", "so", "su", "sd")


def block_step(single_blk, pair_blk, mask_blk, d_single_blk, d_pair_blk, *weights):
    (w1i, w1g, w1o, w2i, w2g, w2o, w3q, w3b, w3o, w4q, w4b, w4o, wpu, wpd, wsq, wsb, wsp, wso, wsu, wsd) = weights
    me = lax.axis_index(GROUP_AXIS)
    idx = jnp.bitwise_xor(me, jnp.arange(4, dtype=jnp.int32))
    z0 = pair_blk[0]
    rows = z0.shape[0]
    mask_add = (mask_blk[0].astype(F32) - 1.0) * MASK_PENALTY
    w1t, w2t, w3bt, w4bt, wspt = w1i.T, w2i.T, w3b.T, w4b.T, wsp.T
    both = lax.all_gather(jnp.stack([single_blk[0], d_single_blk[0]]), GROUP_AXIS, axis=1, tiled=True)

    a1, b1 = mul_pre(z0, w1t)
    b1g = gather_rel(b1)
    x1 = mix_all(functools.partial(mix_fwd, idx), a1, b1g)
    z1 = mul_post(x1, z0, w1g, w1o)
    z1c = rows_to_cols(z1)
    a2r, b2r = mul_pre(z1, w2t)
    a2, b2 = mul_pre(z1c, w2t)
    b2g = gather_rel(b2)
    x2 = mix_all(functools.partial(mix_fwd, idx), a2, b2g)
    z2 = mul_post(x2, z1, w2g, w2o)
    bias3 = bias_full(att_bias(z2, w3bt), mask_add)
    d_cols = rows_to_cols(d_pair_blk[0])
    z3 = att_fwd(z2, bias3, w3q, w3o, 4)
    z3, d_cols = tie(z3, d_cols)
    z3 = rows_to_cols(z3)
    bias4 = bias_full(att_bias(z3, w4bt), mask_add)
    z4 = att_fwd(z3, bias4, w4q, w4o, 4).reshape(-1, C)
    z5 = trans_fwd(z4, wpu, wpd, 1024).reshape(rows, T, C)
    biass = bias_full(att_bias(z5, wspt), mask_add[:, None])

    s_all, ds_all, dbias_s, g_sb, g_sq, g_so, g_su, g_sd = single_step(both[0], both[1], biass, wsq, wsb[None], wso, wsu, wsd)
    s_out = lax.dynamic_slice_in_dim(s_all, me * rows, rows)
    ds_in = lax.dynamic_slice_in_dim(ds_all, me * rows, rows)
    dbias_s = jnp.transpose(lax.dynamic_slice_in_dim(dbias_s, me * rows, rows, 1), (1, 0, 2))
    g_sb = jnp.pad(g_sb.reshape(3, 128), ((0, 5), (0, 0)))
    half_s = group_half([g_sq, g_so, g_su, g_sd, g_sb], False)
    half_s, z5 = tie(half_s, z5)
    part_s = scatter_group(half_s)

    dz5, g_sp = att_fin(z5, d_cols, dbias_s, wspt)
    a1g = gather_rel(a1)
    full_s = gather_group(part_s, False)
    dz4, g_pu, g_pd = trans_bwd(z4, dz5.reshape(-1, C), wpu, wpd, 512)
    dz4 = dz4.reshape(rows, T, C)
    pair_out = cols_to_rows(z5)
    dn4, db4, g_4q, g_4o = att_bwd(z3, dz4, bias4, w4q, w4o, 4)
    db4 = scatter_rows(jnp.transpose(db4, (1, 0, 2)))
    dz3, g_4b = att_fin(z3, dz4, db4, w4bt, dn4)
    half_p = group_half([g_pu, g_pd, g_4q, g_4o, g_4b.reshape(-1, 128), g_sp.reshape(-1, 128)], True)
    dz3 = cols_to_rows(dz3)
    half_p, dz3 = tie(half_p, dz3)
    part_p = scatter_group(half_p)
    dn3, db3, g_3q, g_3o = att_bwd(z2, dz3, bias3, w3q, w3o, 4)
    db3, pair_out = tie(db3, pair_out)
    db3 = scatter_rows(jnp.transpose(db3, (1, 0, 2)))
    dz2, g_3b = att_fin(z2, dz3, db3, w3bt, dn3)
    dx2, dgl2, g_2o = mul_post_bwd(x2, z1, dz2, w2g, w2o, 0)
    dx2 = list(dx2)
    full_p = gather_group(part_p, True)
    dx2g = gather_rel(dx2)
    dab2 = mix_all(functools.partial(mix_bwd_in, idx), dx2g, a2r, b2r)
    dz1, g_2i, g_2g = mul_pre_bwd(z1, dz2, [d[0] for d in dab2], [d[1] for d in dab2], dgl2, w2i, w2t, w2g)
    half_i = group_half([g_3q, g_3o, g_3b.reshape(-1, 128), g_2i, g_2g, g_2o], True)
    dx1, dgl1, g_1o, dxp = mul_post_bwd(x1, z0, dz1, w1g, w1o, 1)
    half_i, dxp = tie(half_i, dxp)
    part_i = scatter_group(half_i)
    dxt = flip(lax.all_to_all(dxp, GROUP_AXIS, 1, 0, tiled=True))
    dab1 = mix_all(functools.partial(mix_bwd_out, idx), dx1, dxt, b1g, a1g)
    full_i = gather_group(part_i, True)
    dz0, g_1i, g_1g = mul_pre_bwd(z0, dz1, [d[0] for d in dab1], [d[1] for d in dab1], dgl1, w1i, w1t, w1g)
    half_o = group_half([g_1i, g_1g, g_1o], True)
    full_o = small_group(half_o)

    halves = [full_s[0].shape[0], full_p[0].shape[0], full_i[0].shape[0], full_o[0].shape[0]]
    at = [0, 0, 0, 0]
    place = {}
    for group, names in enumerate((("sq", "so", "su", "sd", "sb"), ("pu", "pd", "4q", "4o", "4b", "sp"), ("3q", "3o", "3b", "2i", "2g", "2o"), ("1i", "1g", "1o"))):
        for name in names:
            w = dict(zip(ORDER, weights))[name]
            place[name] = (w.size, group, at[group], w.shape[-1] if name in ("3b", "4b", "sp") else 0, halves[group])
            at[group] += -(-w.size // 1024) * 8
    table = [place[name] for name in ORDER]
    grad_flat = assemble(table, (full_s, full_p, full_i, full_o), sum(w.size for w in weights))
    return s_out[None], pair_out[None], ds_in[None], dz0[None], grad_flat


def solution(mesh):
    spec_single = P(BATCH_AXIS, GROUP_AXIS, None)
    spec_pair = P(BATCH_AXIS, GROUP_AXIS, None, None)
    spec_mask = P(BATCH_AXIS, None)

    def block_fn(single_rep, pair_rep, token_mask, d_single_out, d_pair_out, *weights):
        in_specs = (spec_single, spec_pair, spec_mask, spec_single, spec_pair) + tuple(P() for w_item in weights)
        out_specs = (spec_single, spec_pair, spec_single, spec_pair, P(BATCH_AXIS))
        mapped = jax.shard_map(block_step, mesh=mesh, in_specs=in_specs, out_specs=out_specs, check_vma=False)
        return mapped(single_rep, pair_rep, token_mask, d_single_out, d_pair_out, *weights)

    return block_fn
```

```python
import functools
import jax
import jax.numpy as jnp
from jax import lax
from jax.experimental import pallas as pl
from jax.experimental.pallas import tpu as pltpu
from jax.sharding import PartitionSpec as P


BATCH_AXIS = 'dp'
GROUP_AXIS = 'dap'
MASK_PENALTY = 1.0e9
NCH = 4
WORK = 1 << 12

NORM_EPS = 1e-5
F32 = jnp.float32
BF16 = jnp.bfloat16


def mm(a, b):
    return lax.dot_general(a, b, (((1,), (0,)), ((), ())), preferred_element_type=F32)


def mm_nt(a, b):
    return lax.dot_general(a, b, (((1,), (1,)), ((), ())), preferred_element_type=F32)


def mm_tn(a, b):
    return lax.dot_general(a, b, (((0,), (0,)), ((), ())), preferred_element_type=F32)


def row_sum(x):
    return jnp.sum(x, axis=-1, keepdims=True)


def col_sum(x):
    return jnp.sum(x, axis=0, keepdims=True)


def ln_stats(x):
    inv = 1.0 / x.shape[-1]
    c = x - row_sum(x) * inv
    r = lax.rsqrt(row_sum(c * c) * inv + NORM_EPS)
    return c * r, r


def ln_back(dn, xh, r):
    inv = 1.0 / dn.shape[-1]
    m1 = row_sum(dn) * inv
    m2 = row_sum(dn * xh) * inv
    return r * (dn - m1 - xh * m2)


def put_flat(ref, val, row=0):
    n = val.shape[1] // 128
    for t in range(n):
        ref[pl.ds(row + t, val.shape[0], stride=n), :] = val[:, t * 128:(t + 1) * 128]
    return row + val.size // 128


def flat_shape(w):
    return jax.ShapeDtypeStruct((w.size // 128, 128), F32)


def last_step():
    return pl.program_id(0) == pl.num_programs(0) - 1


def sig(x):
    return 1.0 / (1.0 + jnp.exp(-x))


def bias_spec(wbt):
    return pl.BlockSpec((8, wbt.shape[0], T), lambda i: (i, 0, 0))


def bias_shape(r, wbt):
    return jax.ShapeDtypeStruct((r, wbt.shape[0], T), BF16)


def trans_fwd_body(z_ref, wu_ref, wd_ref, wbt_ref, o_ref, b_ref):
    x = z_ref[...].astype(F32)
    xh, _ = ln_stats(x)
    h = mm(xh.astype(BF16), wu_ref[...])
    d = h.shape[1] // 2
    h1 = h[:, :d]
    act = (h1 * sig(h1) * h[:, d:]).astype(BF16)
    o = (x + mm(act, wd_ref[...])).astype(BF16)
    o_ref[...] = o
    for i in range(b_ref.shape[0]):
        b_ref[i] = bias_rows(o[i * T:(i + 1) * T], wbt_ref[...])


def trans_bwd_body(z_ref, g_ref, wu_ref, wd_ref, dz_ref, fu_ref, fd_ref, dwu_ref, dwd_ref):
    @pl.when(pl.program_id(0) == 0)
    def _():
        dwu_ref[...] = jnp.zeros_like(dwu_ref)
        dwd_ref[...] = jnp.zeros_like(dwd_ref)

    x = z_ref[...].astype(F32)
    xh, r = ln_stats(x)
    n = xh.astype(BF16)
    h = mm(n, wu_ref[...])
    d = h.shape[1] // 2
    h1, h2 = h[:, :d], h[:, d:]
    s = sig(h1)
    sl = h1 * s
    act = (sl * h2).astype(BF16)
    g = g_ref[...]
    da = mm_nt(g, wd_ref[...]).astype(BF16).astype(F32)
    dwd_ref[...] += mm_tn(act, g)
    dh1 = (da * h2 * (s + sl * (1.0 - s))).astype(BF16)
    dh2 = (da * sl).astype(BF16)
    dh = jnp.concatenate([dh1, dh2], axis=1)
    dwu_ref[...] += mm_tn(n, dh)
    dn = mm_nt(dh, wu_ref[...])
    dz_ref[...] = (g.astype(F32) + ln_back(dn, xh, r)).astype(BF16)

    @pl.when(last_step())
    def _():
        put_flat(fu_ref, dwu_ref[...])
        put_flat(fd_ref, dwd_ref[...])


def row_spec(b):
    return pl.BlockSpec((b, T, C), lambda i: (i, 0, 0))


def full(a):
    nd = len(a.shape)
    return pl.BlockSpec(a.shape, lambda i: (0,) * nd)


def cp(flops):
    return dict(cost_estimate=pl.CostEstimate(flops=flops, bytes_accessed=1 << 23, transcendentals=0),
                compiler_params=pltpu.CompilerParams(vmem_limit_bytes=60 << 20, dimension_semantics=("arbitrary",)))


def trans_fwd(z, wu, wd, wbt):
    p, c = z.shape
    blk = 8 * T
    spec = pl.BlockSpec((blk, c), lambda i: (i, 0))
    return pl.pallas_call(trans_fwd_body, grid=(p // blk,), in_specs=[spec, full(wu), full(wd), full(wbt)], out_specs=[spec, bias_spec(wbt)],
                          out_shape=[jax.ShapeDtypeStruct((p, c), BF16), bias_shape(p // T, wbt)], name="trans_fwd", **cp(p * c * WORK))(z, wu, wd, wbt)


def trans_bwd(z, g, wu, wd, blk):
    p, c = z.shape
    spec = pl.BlockSpec((blk, c), lambda i: (i, 0))
    return pl.pallas_call(trans_bwd_body, grid=(p // blk,), in_specs=[spec, spec, full(wu), full(wd)],
                          out_specs=[spec, full(flat_shape(wu)), full(flat_shape(wd))],
                          out_shape=[jax.ShapeDtypeStruct((p, c), BF16), flat_shape(wu), flat_shape(wd)],
                          scratch_shapes=[pltpu.VMEM(wu.shape, F32), pltpu.VMEM(wd.shape, F32)],
                          name="trans_bwd", **cp(p * c * WORK))(z, g, wu, wd)


H = 8
D = 32
T = 128
C = 256


def head_masks(width, dim):
    lane = lax.broadcasted_iota(jnp.int32, (1, width), 1)
    return [((lane >= h * dim) & (lane < (h + 1) * dim)).astype(F32).astype(BF16) for h in range(width // dim)]


def pair_setup():
    masks = head_masks(C, D)
    n = H // 2
    lane = lax.broadcasted_iota(jnp.int32, (1, C), 1)
    low = (lane < T).astype(F32).astype(BF16)
    return [a + b for a, b in zip(masks[:n], masks[n:])], [low, 1 - low]


def row_masks():
    row = lax.broadcasted_iota(jnp.int32, (C, 1), 0) // D % (H // 2)
    return [(row == m).astype(F32).astype(BF16) for m in range(H // 2)]


def unpair(x, pairs):
    return sum(x[m * T:(m + 1) * T] * p.astype(F32) for m, p in enumerate(pairs))


def head_tn(x, w, flips):
    xt = x.astype(F32).T.astype(BF16)
    y = mm(jnp.concatenate([xt * f for f in flips], axis=1), w)
    return jnp.concatenate([y[:T, :T], y[T:, T:]]).T.astype(BF16)


def softmax(s):
    e = jnp.exp(s - jnp.max(s, axis=-1, keepdims=True))
    return e * (1.0 / row_sum(e))


def stack_heads(x, masks):
    return jnp.concatenate([x * m for m in masks])


def bias_body(z_ref, wbt_ref, o_ref):
    for i in range(z_ref.shape[0]):
        xh, _ = ln_stats(z_ref[i].astype(F32))
        o_ref[i] = mm_nt(wbt_ref[...], xh.astype(BF16)).astype(BF16)


def att_bias(z3, wbt):
    r, h = z3.shape[0], wbt.shape[0]
    return pl.pallas_call(bias_body, grid=(r // 8,), in_specs=[row_spec(8), full(wbt)],
                          out_specs=pl.BlockSpec((8, h, T), lambda i: (i, 0, 0)),
                          out_shape=jax.ShapeDtypeStruct((r, h, T), BF16), name="att_bias", **cp(r * T * C * WORK))(z3, wbt)


def att_fwd_body(z_ref, bias_ref, wq_ref, wo_ref, o_ref):
    b = z_ref.shape[0]
    pairs, sides = pair_setup()
    x = z_ref[...].reshape(b * T, C).astype(F32)
    xh, _ = ln_stats(x)
    pr = mm(xh.astype(BF16), wq_ref[...])
    gates = sig(pr[:, 3 * C:])
    prb = pr[:, :3 * C].astype(BF16)
    outs = []
    for i in range(b):
        row = prb[i * T:(i + 1) * T]
        q, k, v = row[:, :C], row[:, C:2 * C], row[:, 2 * C:]
        lg = mm_nt(stack_heads(q, pairs), stack_heads(k, sides)) * (D ** -0.5)
        ps = []
        for m in range(len(pairs)):
            s = lg[m * T:(m + 1) * T]
            ps.append(jnp.concatenate([softmax(s[:, :T] + bias_ref[m]), softmax(s[:, T:] + bias_ref[m + len(pairs)])], axis=1).astype(BF16))
        o = unpair(mm(jnp.concatenate(ps), stack_heads(v, sides)), pairs)
        outs.append((gates[i * T:(i + 1) * T] * o).astype(BF16))
    gated = jnp.concatenate(outs)
    o_ref[...] = (x + mm(gated, wo_ref[...])).astype(BF16).reshape(b, T, C)


def att_fwd(z3, bias, wq, wo, b):
    r = z3.shape[0]
    spec = row_spec(b)
    return pl.pallas_call(att_fwd_body, grid=(r // b,), in_specs=[spec, full(bias), full(wq), full(wo)], out_specs=spec,
                          out_shape=jax.ShapeDtypeStruct((r, T, C), BF16), name="att_fwd",
                          **cp(r * T * C * WORK))(z3, bias, wq, wo)


def att_bwd_body(z_ref, g_ref, bias_ref, wq_ref, wo_ref, dn_ref, dbias_ref, fq_ref, fo_ref, dwq_ref, dwo_ref):
    @pl.when(pl.program_id(0) == 0)
    def _():
        dbias_ref[...] = jnp.zeros_like(dbias_ref)
        dwq_ref[...] = jnp.zeros_like(dwq_ref)
        dwo_ref[...] = jnp.zeros_like(dwo_ref)

    b = z_ref.shape[0]
    pairs, sides = pair_setup()
    flips = row_masks()
    x = z_ref[...].reshape(b * T, C).astype(F32)
    g = g_ref[...].reshape(b * T, C)
    xh, _ = ln_stats(x)
    n = xh.astype(BF16)
    pr = mm(n, wq_ref[...])
    gates = sig(pr[:, 3 * C:])
    prb = pr[:, :3 * C].astype(BF16)
    dgd = mm_nt(g, wo_ref[...]).astype(BF16).astype(F32)
    do_all = (dgd * gates).astype(BF16)
    gat, dps = [], []
    for i in range(b):
        sl = slice(i * T, (i + 1) * T)
        row = prb[sl]
        q, k, v = row[:, :C], row[:, C:2 * C], row[:, 2 * C:]
        do = do_all[sl]
        qs, dos = stack_heads(q, pairs), stack_heads(do, pairs)
        kk, vv = stack_heads(k, sides), stack_heads(v, sides)
        lg = mm_nt(qs, kk) * (D ** -0.5)
        dp = mm_nt(dos, vv)
        ps, ds = [], []
        for m in range(len(pairs)):
            pp, dd = [], []
            for e in range(2):
                h = m + e * len(pairs)
                blk = (slice(m * T, (m + 1) * T), slice(e * T, (e + 1) * T))
                p = softmax(lg[blk] + bias_ref[h])
                pd = p * dp[blk].astype(BF16).astype(F32)
                dsh = pd - p * row_sum(pd)
                dbias_ref[h] += dsh
                pp.append(p.astype(BF16))
                dd.append((dsh * (D ** -0.5)).astype(BF16))
            ps.append(jnp.concatenate(pp, axis=1))
            ds.append(jnp.concatenate(dd, axis=1))
        ps, ds = jnp.concatenate(ps), jnp.concatenate(ds)
        o = unpair(mm(ps, vv), pairs)
        dq = unpair(mm(ds, kk), pairs).astype(BF16)
        dk, dv = head_tn(q, ds, flips), head_tn(do, ps, flips)
        gt = gates[sl]
        gat.append((gt * o).astype(BF16))
        dgl = (dgd[sl] * o * gt * (1.0 - gt)).astype(BF16)
        dps.append(jnp.concatenate([dq, dk, dv, dgl], axis=1))
    gated = jnp.concatenate(gat)
    dpr = jnp.concatenate(dps)
    dwo_ref[...] += mm_tn(gated, g)
    dwq_ref[...] += mm_tn(n, dpr)
    dn_ref[...] = mm_nt(dpr, wq_ref[...])

    @pl.when(last_step())
    def _():
        put_flat(fq_ref, dwq_ref[...])
        put_flat(fo_ref, dwo_ref[...])


def att_bwd(z3, g3, bias, wq, wo, b):
    r = z3.shape[0]
    spec = row_spec(b)
    return pl.pallas_call(att_bwd_body, grid=(r // b,), in_specs=[spec, spec, full(bias), full(wq), full(wo)],
                          out_specs=[pl.BlockSpec((b * T, C), lambda i: (i, 0)), full(bias), full(flat_shape(wq)), full(flat_shape(wo))],
                          out_shape=[jax.ShapeDtypeStruct((r * T, C), F32), jax.ShapeDtypeStruct(bias.shape, F32), flat_shape(wq), flat_shape(wo)],
                          scratch_shapes=[pltpu.VMEM(wq.shape, F32), pltpu.VMEM(wo.shape, F32)],
                          name="att_bwd", **cp(r * T * C * WORK))(z3, g3, bias, wq, wo)


def att_fin_body(z_ref, g_ref, db_ref, wbt_ref, *rest):
    dz_ref, dwbt_ref = rest[-2:]

    @pl.when(pl.program_id(0) == 0)
    def _():
        dwbt_ref[...] = jnp.zeros_like(dwbt_ref)

    b = z_ref.shape[0]
    xh, r = ln_stats(z_ref[...].reshape(b * T, C).astype(F32))
    n = xh.astype(BF16)
    parts = []
    for i in range(b):
        db = db_ref[i].astype(BF16)
        parts.append(mm_tn(db, wbt_ref[...]))
        dwbt_ref[...] += mm(db, n[i * T:(i + 1) * T])
    dn = jnp.concatenate(parts)
    if len(rest) == 3:
        dn = dn + rest[0][...]
    dz_ref[...] = (g_ref[...].reshape(b * T, C).astype(F32) + ln_back(dn, xh, r)).astype(BF16).reshape(b, T, C)


def att_fin(z3, g3, db, wbt, dn=None):
    r, h = z3.shape[0], wbt.shape[0]
    b = 8
    spec = row_spec(b)
    extra = [] if dn is None else [dn]
    return pl.pallas_call(att_fin_body, grid=(r // b,),
                          in_specs=[spec, spec, pl.BlockSpec((b, h, T), lambda i: (i, 0, 0)), full(wbt)]
                          + [pl.BlockSpec((b * T, C), lambda i: (i, 0))] * len(extra),
                          out_specs=[spec, full(wbt)],
                          out_shape=[jax.ShapeDtypeStruct((r, T, C), BF16), jax.ShapeDtypeStruct(wbt.shape, F32)],
                          name="att_fin", **cp(r * T * C * WORK))(z3, g3, db, wbt, *extra)


RB = 16
CB = 32


def put_row(scr, i, val):
    scr[pl.ds(i, val.shape[0], stride=RB), :] = val


def get_row(scr, i, n):
    return scr[pl.ds(i, n, stride=RB), :]


def cspecs(n):
    return [pl.BlockSpec((C // n, RB, T), lambda i: (0, i, 0))] * n


def cshapes(n, r, dt=BF16):
    return [jax.ShapeDtypeStruct((C // n, r, T), dt)] * n


def flush(scr, refs):
    w = C // len(refs)
    for p, ref in enumerate(refs):
        ref[...] = scr[pl.ds(p * w * RB, w * RB), :].reshape(w, RB, T).astype(BF16)


def mul_pre_body(z_ref, wt_ref, *rest):
    outs, sa, sb = rest[:-2], rest[-2], rest[-1]
    wt = wt_ref[...]
    for i in range(0, RB, 2):
        xh, _ = ln_stats(z_ref[i:i + 2].reshape(2 * T, C).astype(F32))
        pt = mm_nt(wt, xh.astype(BF16))
        at = sig(pt[C:2 * C]) * pt[:C]
        bt = sig(pt[3 * C:]) * pt[2 * C:3 * C]
        for e in range(2):
            put_row(sa, i + e, at[:, e * T:(e + 1) * T])
            put_row(sb, i + e, bt[:, e * T:(e + 1) * T])
    flush(sa, outs[:NCH])
    flush(sb, outs[NCH:])


def mul_pre(z3, wt):
    r = z3.shape[0]
    zs = row_spec(RB)
    out = pl.pallas_call(mul_pre_body, grid=(r // RB,), in_specs=[zs, full(wt)], out_specs=cspecs(NCH) * 2, out_shape=cshapes(NCH, r) * 2,
                         scratch_shapes=[pltpu.VMEM((C * RB, T), F32)] * 2, name="mul_pre", **cp(r * T * C * WORK))(z3, wt)
    return out[:NCH], out[NCH:]


def collect(idx_ref, refs, buf):
    for rel, ref in enumerate(refs):
        r = ref.shape[1]
        buf[:, pl.ds(pl.multiple_of(idx_ref[rel] * r, r), r), :] = ref[...]


def mix_call(body, idx, ins, n_out, out_dt, n_buf):
    w, r, _ = ins[0].shape
    spec = pl.BlockSpec((CB, r, T), lambda i, s: (i, 0, 0))
    gs = pltpu.PrefetchScalarGridSpec(num_scalar_prefetch=1, grid=(w // CB,), in_specs=[spec] * len(ins), out_specs=[spec] * n_out,
                                      scratch_shapes=[pltpu.VMEM((CB, T, T), BF16)] * n_buf)
    return pl.pallas_call(body, grid_spec=gs, out_shape=[jax.ShapeDtypeStruct((w, r, T), out_dt)] * n_out, **cp(r * w * T * WORK))(idx, *ins)


def mix_fwd_body(idx_ref, a_ref, b0, b1, b2, b3, x_ref, buf):
    collect(idx_ref, (b0, b1, b2, b3), buf)
    for c in range(CB):
        x_ref[c] = mm_nt(a_ref[c], buf[c])


def mix_fwd(idx, a, b4):
    return mix_call(mix_fwd_body, idx, [a, *b4], 1, F32, 1)[0]


def mix_nn_body(idx_ref, x_ref, b0, b1, b2, b3, o_ref, buf):
    collect(idx_ref, (b0, b1, b2, b3), buf)
    for c in range(CB):
        o_ref[c] = mm(x_ref[c], buf[c]).astype(BF16)


def mix_nn(idx, x, b4):
    return mix_call(mix_nn_body, idx, [x, *b4], 1, BF16, 1)[0]


def mix_bwd_in_body(idx_ref, a_ref, b_ref, d0, d1, d2, d3, da_ref, db_ref, buf):
    collect(idx_ref, (d0, d1, d2, d3), buf)
    for c in range(CB):
        d = buf[c]
        da_ref[c] = mm_nt(b_ref[c], d).astype(BF16)
        db_ref[c] = mm(a_ref[c], d).astype(BF16)


def mix_bwd_in(idx, d4, a, b):
    return mix_call(mix_bwd_in_body, idx, [a, b, *d4], 2, BF16, 1)


def ln0_stats(x):
    inv = 1.0 / x.shape[0]
    c = x - col_sum(x) * inv
    r = lax.rsqrt(col_sum(c * c) * inv + NORM_EPS)
    return c * r, r


def ln0_back(dn, xh, r):
    inv = 1.0 / dn.shape[0]
    m1 = col_sum(dn) * inv
    m2 = col_sum(dn * xh) * inv
    return r * (dn - m1 - xh * m2)


def col_of(refs, i):
    return jnp.concatenate([ref[:, i, :] for ref in refs])


def bias_rows(x, wbt):
    xh, _ = ln_stats(x.astype(F32))
    return mm_nt(wbt, xh.astype(BF16)).astype(BF16)


def mul_post_body(*refs):
    xs, (z_ref, wg_ref, wo_ref), rest = refs[:NCH], refs[NCH:NCH + 3], refs[NCH + 3:]
    wbt_ref, o_ref, b_ref = rest if len(rest) == 3 else (None, *rest, None)
    for i in range(z_ref.shape[0]):
        z = z_ref[i].astype(F32)
        n, _ = ln_stats(z)
        g = sig(mm(n.astype(BF16), wg_ref[...]))
        xn, _ = ln0_stats(col_of(xs, i))
        o = (z + g * mm_tn(xn.astype(BF16), wo_ref[...])).astype(BF16)
        o_ref[i] = o
        if wbt_ref is not None:
            b_ref[i] = bias_rows(o, wbt_ref[...])


def mul_post(xs, z3, wg, wo, *wbt):
    r = z3.shape[0]
    b = 8
    zs = row_spec(b)
    xspec = pl.BlockSpec((C // NCH, b, T), lambda i: (0, i, 0))
    return pl.pallas_call(mul_post_body, grid=(r // b,), in_specs=[xspec] * NCH + [zs, full(wg), full(wo)] + [full(w) for w in wbt],
                          out_specs=[zs] + [bias_spec(w) for w in wbt], out_shape=[jax.ShapeDtypeStruct((r, T, C), BF16)] + [bias_shape(r, w) for w in wbt], name="mul_post", **cp(r * T * C * WORK))(*xs, z3, wg, wo, *wbt)


def mul_post_bwd_body(pix, *refs):
    xs, (z_ref, d_ref, wg_ref, wo_ref) = refs[:NCH], refs[NCH:NCH + 4]
    dxs, (dgl_ref, fo_ref) = refs[NCH + 4:2 * NCH + 4], refs[2 * NCH + 4:2 * NCH + 6]
    scr, dwo_ref = refs[-2:]

    @pl.when(pl.program_id(0) == 0)
    def _():
        dwo_ref[...] = jnp.zeros_like(dwo_ref)

    for i in range(RB):
        n, _ = ln_stats(z_ref[i].astype(F32))
        g = sig(mm(n.astype(BF16), wg_ref[...]))
        xh, r = ln0_stats(col_of(xs, i))
        xn = xh.astype(BF16)
        u = mm_tn(xn, wo_ref[...])
        d = d_ref[i].astype(F32)
        du = (d * g).astype(BF16)
        dgl_ref[i] = (d * u * g * (1.0 - g)).astype(BF16)
        dwo_ref[...] += mm(xn, du)
        dx = ln0_back(mm_nt(wo_ref[...], du), xh, r)
        put_row(scr, i, dx)
        if pix:
            refs[2 * NCH + 6][i] = dx.T.astype(BF16)
    flush(scr, dxs)

    @pl.when(last_step())
    def _():
        put_flat(fo_ref, dwo_ref[...])


def mul_post_bwd(xs, z3, d3, wg, wo, pix):
    r = z3.shape[0]
    zs = row_spec(RB)
    zsh = jax.ShapeDtypeStruct((r, T, C), BF16)
    out = pl.pallas_call(functools.partial(mul_post_bwd_body, pix), grid=(r // RB,), in_specs=cspecs(NCH) + [zs, zs, full(wg), full(wo)],
                         out_specs=cspecs(NCH) + [zs, full(flat_shape(wo))] + [zs] * pix,
                         out_shape=cshapes(NCH, r) + [zsh, flat_shape(wo)] + [zsh] * pix,
                         scratch_shapes=[pltpu.VMEM((C * RB, T), F32), pltpu.VMEM(wo.shape, F32)],
                         name="mul_post_bwd", **cp(r * T * C * WORK))(*xs, z3, d3, wg, wo)
    return (out[:NCH], *out[NCH:])


def flip_body(d_ref, *rest):
    sin, sout = rest[-2:]
    for hf in range(2):
        sin[hf] = d_ref[:, :, hf * T:(hf + 1) * T].astype(F32).reshape(T * RB, T)
    for j in range(RB):
        for hf in range(2):
            m = sin[hf, pl.ds(j, T, stride=RB), :]
            sout[pl.ds(hf * T * RB + j, T, stride=RB), :] = m.T
    flush(sout, rest[:-2])


def flip(d):
    r = d.shape[1]
    return pl.pallas_call(flip_body, grid=(r // RB,), in_specs=[pl.BlockSpec((T, RB, C), lambda i: (0, i, 0))],
                          out_specs=cspecs(NCH), out_shape=cshapes(NCH, r),
                          scratch_shapes=[pltpu.VMEM((2, T * RB, T), F32), pltpu.VMEM((C * RB, T), F32)], name="flip", **cp(r * T * C * WORK))(d)


def load_all(scr, refs):
    w = C // len(refs)
    for p, ref in enumerate(refs):
        scr[pl.ds(p * w * RB, w * RB), :] = ref[...].astype(F32).reshape(w * RB, T)


def mul_pre_bwd_body(*refs):
    das, dbs = refs[:NCH], refs[NCH:2 * NCH]
    z_ref, g_ref, dgl_ref, w_ref, wt_ref, wg_ref, dz_ref, fi_ref, fg_ref, sa, sb, dwt_ref, dwg_ref = refs[2 * NCH:]

    @pl.when(pl.program_id(0) == 0)
    def _():
        dwt_ref[...] = jnp.zeros_like(dwt_ref)
        dwg_ref[...] = jnp.zeros_like(dwg_ref)

    load_all(sa, das)
    load_all(sb, dbs)
    for i in range(0, RB, 2):
        xh, r = ln_stats(z_ref[i:i + 2].reshape(2 * T, C).astype(F32))
        n = xh.astype(BF16)
        pt = mm_nt(wt_ref[...], n)
        da = jnp.concatenate([get_row(sa, i, C), get_row(sa, i + 1, C)], axis=1)
        db = jnp.concatenate([get_row(sb, i, C), get_row(sb, i + 1, C)], axis=1)
        s1, s2 = sig(pt[C:2 * C]), sig(pt[3 * C:])
        d1, d3 = da * s1, db * s2
        dp = jnp.concatenate([d1.astype(BF16), (d1 * pt[:C] * (1.0 - s1)).astype(BF16),
                              d3.astype(BF16), (d3 * pt[2 * C:3 * C] * (1.0 - s2)).astype(BF16)])
        dgl = dgl_ref[i:i + 2].reshape(2 * T, C)
        dwt_ref[...] += mm(dp, n)
        dwg_ref[...] += mm_tn(n, dgl)
        dn = mm(w_ref[...], dp).T + mm_nt(dgl, wg_ref[...])
        dz = g_ref[i:i + 2].reshape(2 * T, C).astype(F32) + ln_back(dn, xh, r)
        dz_ref[i:i + 2] = dz.astype(BF16).reshape(2, T, C)

    @pl.when(last_step())
    def _():
        put_flat(fi_ref, dwt_ref[...].T)
        put_flat(fg_ref, dwg_ref[...])


def mul_pre_bwd(z3, g3, das, dbs, dgl, w, wt, wg):
    r = z3.shape[0]
    zs = row_spec(RB)
    return pl.pallas_call(mul_pre_bwd_body, grid=(r // RB,), in_specs=cspecs(NCH) * 2 + [zs, zs, zs, full(w), full(wt), full(wg)],
                          out_specs=[zs, full(flat_shape(wt)), full(flat_shape(wg))],
                          out_shape=[jax.ShapeDtypeStruct((r, T, C), BF16), flat_shape(wt), flat_shape(wg)],
                          scratch_shapes=[pltpu.VMEM((C * RB, T), F32)] * 2 + [pltpu.VMEM(wt.shape, F32), pltpu.VMEM(wg.shape, F32)],
                          name="mul_pre_bwd", **cp(r * T * C * WORK))(*das, *dbs, z3, g3, dgl, w, wt, wg)


SH = 16
SD = 24


def single_body(s_ref, d_ref, bias_ref, wq_ref, qb_ref, wo_ref, wu_ref, wd_ref,
                so_ref, ds_ref, dbias_ref, flat_ref):
    w = s_ref.shape[1]
    masks = head_masks(w, SD)
    x = s_ref[...].astype(F32)
    xh, r = ln_stats(x)
    n = xh.astype(BF16)
    pr = mm(n, wq_ref[...])
    q = (pr[:, :w] + qb_ref[...].astype(F32)).astype(BF16)
    k = pr[:, w:2 * w].astype(BF16)
    v = pr[:, 2 * w:3 * w].astype(BF16)
    gt = sig(pr[:, 3 * w:])
    qs = stack_heads(q, masks)
    lg = mm_nt(qs, k) * (SD ** -0.5)
    pf, ps = [], []
    for h in range(SH):
        p = softmax(lg[h * T:(h + 1) * T] + bias_ref[h].T)
        pf.append(p)
        ps.append(p.astype(BF16))
    o = mm(jnp.concatenate(ps, axis=1), stack_heads(v, masks))
    gated = (gt * o).astype(BF16)
    s1 = (x + mm(gated, wo_ref[...])).astype(BF16)
    x1 = s1.astype(F32)
    xh1, r1 = ln_stats(x1)
    n1 = xh1.astype(BF16)
    hid = mm(n1, wu_ref[...])
    d = hid.shape[1] // 2
    h1, h2 = hid[:, :d], hid[:, d:]
    sg = sig(h1)
    sl = h1 * sg
    act = (sl * h2).astype(BF16)
    so_ref[...] = (x1 + mm(act, wd_ref[...])).astype(BF16)
    g = d_ref[...]
    da = mm_nt(g, wd_ref[...]).astype(BF16).astype(F32)
    g_wd = mm_tn(act, g)
    dh = jnp.concatenate([(da * h2 * (sg + sl * (1.0 - sg))).astype(BF16), (da * sl).astype(BF16)], axis=1)
    g_wu = mm_tn(n1, dh)
    g1 = (g.astype(F32) + ln_back(mm_nt(dh, wu_ref[...]), xh1, r1)).astype(BF16)
    dgd = mm_nt(g1, wo_ref[...]).astype(BF16).astype(F32)
    g_wo = mm_tn(gated, g1)
    do = (dgd * gt).astype(BF16)
    dgl = (dgd * o * gt * (1.0 - gt)).astype(BF16)
    dos = stack_heads(do, masks)
    dp = mm_nt(dos, v)
    ds = []
    for h in range(SH):
        pd = pf[h] * dp[h * T:(h + 1) * T].astype(BF16).astype(F32)
        dsh = pd - pf[h] * row_sum(pd)
        dbias_ref[h] = dsh.T
        ds.append((dsh * (SD ** -0.5)).astype(BF16))
    dq = mm(jnp.concatenate(ds, axis=1), stack_heads(k, masks)).astype(BF16)
    dk = mm_tn(jnp.concatenate(ds), qs).astype(BF16)
    dv = mm_tn(jnp.concatenate(ps), dos).astype(BF16)
    dpr = jnp.concatenate([dq, dk, dv, dgl], axis=1)
    row = 0
    for val in (mm_tn(n, dpr), g_wo, g_wu, g_wd):
        row = put_flat(flat_ref, val, row)
    flat_ref[pl.ds(row, flat_ref.shape[0] - row), :] = jnp.zeros((flat_ref.shape[0] - row, 128), F32)
    put_flat(flat_ref, col_sum(dq.astype(F32)), row)
    ds_ref[...] = (g1.astype(F32) + ln_back(mm_nt(dpr, wq_ref[...]), xh, r)).astype(BF16)


def single_step(s, d, bias, wq, qb, wo, wu, wd):
    vm = pl.BlockSpec(memory_space=pltpu.VMEM)
    rows = sum(-(-a.size // (128 * 128)) for a in (wq, qb, wo, wu, wd)) * 128
    sh = [jax.ShapeDtypeStruct(s.shape, BF16)] * 2 + [jax.ShapeDtypeStruct(bias.shape, F32), jax.ShapeDtypeStruct((rows, 128), F32)]
    return pl.pallas_call(single_body, in_specs=[vm] * 8, out_specs=[vm] * 4, out_shape=sh, name="single_step",
                          cost_estimate=pl.CostEstimate(flops=1 << 33, bytes_accessed=1 << 24, transcendentals=0),
                          compiler_params=pltpu.CompilerParams(vmem_limit_bytes=60 << 20))(s, d, bias, wq, qb, wo, wu, wd)


def flip_perm(bit):
    return [(i, i ^ bit) for i in range(4)]


def swap_core(x_in):
    return lax.ppermute(x_in, GROUP_AXIS, flip_perm(1))


def swap_chip(x_in):
    return lax.ppermute(x_in, GROUP_AXIS, flip_perm(2))


def gather_rel(xs):
    out = []
    for x_in in xs:
        near = swap_core(x_in)
        far = swap_chip(x_in)
        out.append((x_in, near, far, swap_core(far)))
    return out


def mix_all(fn, *chunks):
    out = []
    for args in zip(*chunks):
        out.append(fn(*args))
    return out


def rows_to_cols(x_in):
    return jnp.transpose(lax.all_to_all(x_in, GROUP_AXIS, 1, 0, tiled=True), (1, 0, 2))


def cols_to_rows(x_in):
    return lax.all_to_all(jnp.transpose(x_in, (1, 0, 2)), GROUP_AXIS, 0, 1, tiled=True)


def scatter_rows(x_in):
    me = lax.axis_index(GROUP_AXIS)
    chip, core = me // 2, me % 2
    halves = x_in.reshape((2, 2) + (x_in.shape[0] // 4,) + x_in.shape[1:])
    mine = lax.dynamic_index_in_dim(halves, chip, 0, keepdims=False)
    mine = mine + swap_chip(lax.dynamic_index_in_dim(halves, 1 - chip, 0, keepdims=False))
    own = lax.dynamic_index_in_dim(mine, core, 0, keepdims=False)
    return own + swap_core(lax.dynamic_index_in_dim(mine, 1 - core, 0, keepdims=False))


def bias_full(part, mask_add):
    return jnp.transpose(lax.all_gather(part, GROUP_AXIS, axis=0, tiled=True), (1, 0, 2)).astype(F32) + mask_add


def group_half(pieces, partial):
    core = lax.axis_index(GROUP_AXIS) % 2
    rows = sum(p.shape[0] for p in pieces)
    pad = -rows % 128
    flat = jnp.concatenate(list(pieces) + ([jnp.zeros((pad, 128), F32)] if pad else []), axis=0)
    half = flat.shape[0] // 2
    mine = lax.dynamic_slice_in_dim(flat, core * half, half)
    if partial:
        mine = mine + swap_core(lax.dynamic_slice_in_dim(flat, (1 - core) * half, half))
    return mine


def scatter_group(mine):
    return lax.psum_scatter(mine, BATCH_AXIS, scatter_dimension=0, tiled=True)


def gather_group(part, partial):
    if partial:
        part = part + swap_chip(part)
    got = lax.all_gather(part, BATCH_AXIS, axis=0, tiled=True)
    return got, swap_core(got)


def dp_perm(bit):
    n = lax.axis_size(BATCH_AXIS)
    return [(i, i ^ bit) for i in range(n)]


def small_group(mine):
    me = lax.axis_index(BATCH_AXIS)
    bits = (1, 2, 4)
    for bit in bits:
        half = mine.shape[0] // 2
        side = (me // bit) % 2
        other = lax.ppermute(lax.dynamic_slice_in_dim(mine, (1 - side) * half, half), BATCH_AXIS, dp_perm(bit))
        mine = lax.dynamic_slice_in_dim(mine, side * half, half) + other
    mine = mine + swap_chip(mine)
    for bit in reversed(bits):
        half = mine.shape[0]
        side = (me // bit) % 2
        other = lax.ppermute(mine, BATCH_AXIS, dp_perm(bit))
        both = jnp.zeros((2 * half, 128), F32)
        both = lax.dynamic_update_slice_in_dim(both, mine, side * half, 0)
        mine = lax.dynamic_update_slice_in_dim(both, other, (1 - side) * half, 0)
    return mine, swap_core(mine)


def chunk_pieces(table, start, size, core):
    at, out = 0, []
    for elems, group, row, flip_dim, half in table:
        lo, hi = max(at, start), min(at + elems, start + size)
        if lo < hi:
            cut = half * 128
            a, b = row * 128 + lo - at, row * 128 + hi - at
            if flip_dim:
                a, b = row * 128, row * 128 + elems
            spans = [(a, min(b, cut)), (max(a, cut), b)]
            segs = [(group, int((base >= cut) != (core == 1)), base % cut, end - base) for base, end in spans if base < end]
            out.append((segs, flip_dim, lo - at, hi - at))
        at += elems
    return out


def assemble(table, groups, total):
    n = lax.axis_size(BATCH_AXIS)
    part = total // n

    def branch(d, core):
        def run(*flat_groups):
            res = []
            for segs, flip_dim, lo, hi in chunk_pieces(table, d * part, part, core):
                vals = [flat_groups[2 * g + side].reshape(-1)[o:o + ln] for g, side, o, ln in segs]
                if flip_dim:
                    val = jnp.concatenate(vals).reshape(flip_dim, -1).T.reshape(-1)
                    vals = [val[lo:hi]]
                res += vals
            return jnp.concatenate(res)

        return run

    which = lax.axis_index(BATCH_AXIS) * 2 + lax.axis_index(GROUP_AXIS) % 2
    flat_groups = [a for g in groups for a in g]
    return lax.switch(which, [branch(d, c) for d in range(n) for c in range(2)], *flat_groups)


def tie(*vals):
    return lax.optimization_barrier(vals)


ORDER = ("1i", "1g", "1o", "2i", "2g", "2o", "3q", "3b", "3o", "4q", "4b", "4o", "pu", "pd", "sq", "sb", "sp", "so", "su", "sd")


def block_step(single_blk, pair_blk, mask_blk, d_single_blk, d_pair_blk, *weights):
    (w1i, w1g, w1o, w2i, w2g, w2o, w3q, w3b, w3o, w4q, w4b, w4o, wpu, wpd, wsq, wsb, wsp, wso, wsu, wsd) = weights
    me = lax.axis_index(GROUP_AXIS)
    idx = jnp.bitwise_xor(me, jnp.arange(4, dtype=jnp.int32))
    z0 = pair_blk[0]
    rows = z0.shape[0]
    mask_add = (mask_blk[0].astype(F32) - 1.0) * MASK_PENALTY
    w1t, w2t, w3bt, w4bt, wspt = w1i.T, w2i.T, w3b.T, w4b.T, wsp.T
    both = lax.all_gather(jnp.stack([single_blk[0], d_single_blk[0]]), GROUP_AXIS, axis=1, tiled=True)

    a1, b1 = mul_pre(z0, w1t)
    b1g = gather_rel(b1)
    x1 = mix_all(functools.partial(mix_fwd, idx), a1, b1g)
    z1 = mul_post(x1, z0, w1g, w1o)[0]
    z1c = rows_to_cols(z1)
    a2r, b2r = mul_pre(z1, w2t)
    a2, b2 = mul_pre(z1c, w2t)
    b2g = gather_rel(b2)
    x2 = mix_all(functools.partial(mix_fwd, idx), a2, b2g)
    z2, bias_z2 = mul_post(x2, z1, w2g, w2o, w3bt)
    bias3 = bias_full(bias_z2, mask_add)
    d_cols = rows_to_cols(d_pair_blk[0])
    z3 = att_fwd(z2, bias3, w3q, w3o, 4)
    z3, d_cols = tie(z3, d_cols)
    z3 = rows_to_cols(z3)
    bias4 = bias_full(att_bias(z3, w4bt), mask_add)
    z4 = att_fwd(z3, bias4, w4q, w4o, 4).reshape(-1, C)
    z5, bias_z5 = trans_fwd(z4, wpu, wpd, wspt)
    z5 = z5.reshape(rows, T, C)
    biass = bias_full(bias_z5, mask_add[:, None])

    s_all, ds_all, dbias_s, g_s = single_step(both[0], both[1], biass, wsq, wsb[None], wso, wsu, wsd)
    s_out = lax.dynamic_slice_in_dim(s_all, me * rows, rows)
    ds_in = lax.dynamic_slice_in_dim(ds_all, me * rows, rows)
    dbias_s = jnp.transpose(lax.dynamic_slice_in_dim(dbias_s, me * rows, rows, 1), (1, 0, 2))
    half_s = group_half([g_s], False)
    half_s, z5 = tie(half_s, z5)
    part_s = scatter_group(half_s)

    dz5, g_sp = att_fin(z5, d_cols, dbias_s, wspt)
    a1g = gather_rel(a1)
    full_s = gather_group(part_s, False)
    dz4, g_pu, g_pd = trans_bwd(z4, dz5.reshape(-1, C), wpu, wpd, 512)
    dz4 = dz4.reshape(rows, T, C)
    pair_out = cols_to_rows(z5)
    dn4, db4, g_4q, g_4o = att_bwd(z3, dz4, bias4, w4q, w4o, 4)
    db4 = scatter_rows(jnp.transpose(db4, (1, 0, 2)))
    dz3, g_4b = att_fin(z3, dz4, db4, w4bt, dn4)
    half_p = group_half([g_pu, g_pd, g_4q, g_4o, g_4b.reshape(-1, 128), g_sp.reshape(-1, 128)], True)
    dz3 = cols_to_rows(dz3)
    half_p, dz3 = tie(half_p, dz3)
    part_p = scatter_group(half_p)
    dn3, db3, g_3q, g_3o = att_bwd(z2, dz3, bias3, w3q, w3o, 4)
    db3, pair_out = tie(db3, pair_out)
    db3 = scatter_rows(jnp.transpose(db3, (1, 0, 2)))
    dz2, g_3b = att_fin(z2, dz3, db3, w3bt, dn3)
    dx2, dgl2, g_2o = mul_post_bwd(x2, z1, dz2, w2g, w2o, 0)
    dx2 = list(dx2)
    full_p = gather_group(part_p, True)
    dx2g = gather_rel(dx2)
    dab2 = mix_all(functools.partial(mix_bwd_in, idx), dx2g, a2r, b2r)
    dz1, g_2i, g_2g = mul_pre_bwd(z1, dz2, [d[0] for d in dab2], [d[1] for d in dab2], dgl2, w2i, w2t, w2g)
    half_i = group_half([g_3q, g_3o, g_3b.reshape(-1, 128), g_2i, g_2g, g_2o], True)
    dx1, dgl1, g_1o, dxp = mul_post_bwd(x1, z0, dz1, w1g, w1o, 1)
    half_i, dxp = tie(half_i, dxp)
    part_i = scatter_group(half_i)
    dxt = lax.all_to_all(dxp, GROUP_AXIS, 1, 0, tiled=True)
    da1 = mix_all(functools.partial(mix_nn, idx), dx1, b1g)
    db1 = mix_all(functools.partial(mix_nn, idx), flip(dxt), a1g)
    full_i = gather_group(part_i, True)
    dz0, g_1i, g_1g = mul_pre_bwd(z0, dz1, da1, db1, dgl1, w1i, w1t, w1g)
    half_o = group_half([g_1i, g_1g, g_1o], True)
    full_o = small_group(half_o)

    halves = [full_s[0].shape[0], full_p[0].shape[0], full_i[0].shape[0], full_o[0].shape[0]]
    at = [0, 0, 0, 0]
    place = {}
    for group, names in enumerate((("sq", "so", "su", "sd", "sb"), ("pu", "pd", "4q", "4o", "4b", "sp"), ("3q", "3o", "3b", "2i", "2g", "2o"), ("1i", "1g", "1o"))):
        for name in names:
            w = dict(zip(ORDER, weights))[name]
            place[name] = (w.size, group, at[group], w.shape[-1] if name in ("3b", "4b", "sp") else 0, halves[group])
            at[group] += -(-w.size // 1024) * 8
    table = [place[name] for name in ORDER]
    grad_flat = assemble(table, (full_s, full_p, full_i, full_o), sum(w.size for w in weights))
    return s_out[None], pair_out[None], ds_in[None], dz0[None], grad_flat


def solution(mesh):
    spec_single = P(BATCH_AXIS, GROUP_AXIS, None)
    spec_pair = P(BATCH_AXIS, GROUP_AXIS, None, None)
    spec_mask = P(BATCH_AXIS, None)

    def block_fn(single_rep, pair_rep, token_mask, d_single_out, d_pair_out, *weights):
        in_specs = (spec_single, spec_pair, spec_mask, spec_single, spec_pair) + tuple(P() for w_item in weights)
        out_specs = (spec_single, spec_pair, spec_single, spec_pair, P(BATCH_AXIS))
        mapped = jax.shard_map(block_step, mesh=mesh, in_specs=in_specs, out_specs=out_specs, check_vma=False)
        return mapped(single_rep, pair_rep, token_mask, d_single_out, d_pair_out, *weights)

    return block_fn
```
